128 devices in a mesh: seq: 16 (over y, x), head: 8 (over z, core).
Axes of the slice: x: 4, y: 4, z: 4, core: 2. Of those that a mesh axis runs over, the one named last changes fastest.
Arguments:
- segment_input: bfloat16 [2, 4096, 3584], P(None, 'seq'), may hold values from -16 to 16
- doc_ids: int32 [2, 4096], replicated, may hold values from 0 to 3, never falling along the last dimension, each value on 1 to 2048 neighbouring positions
- memory: bfloat16 [32, 3584], replicated, may hold values from -16 to 16
- gain: bfloat16 [3584], replicated, may hold values from 0.099609375 to 1.8984375
- w_query: bfloat16 [3584, 4096], P(None, 'head'), may hold values from -4 to 4
- w_key: bfloat16 [3584, 2048], P(None, 'head'), may hold values from -4 to 4
- w_value: bfloat16 [3584, 2048], P(None, 'head'), may hold values from -0.09375 to 0.09375
- w_out: bfloat16 [4096, 3584], P(None, 'head'), may hold values from -0.09375 to 0.09375
- mem_proj: bfloat16 [3584, 3584], P('head'), may hold values from -4 to 4
Outputs:
- hidden: bfloat16 [2, 4096, 3584], P(None, 'seq', 'head')
- new_memory: bfloat16 [32, 3584], replicated
The draws below stay inside these ranges and needn't reach their ends.
Inputs may be any that keep to these rules, and one draw needn't show every extreme that they name: `doc_ids`: ids never fall along a segment; each document has 1 to 2048 tokens.
All inputs are finite; a program needn't handle non-finite values.
Results may differ from the reference program's by a relative error of at most 0.02.
Values may be sent and summed in bfloat16 or wider, within the bound.
A program may use at most 128 MiB of HBM per device.

```python
import math
import jax
import jax.numpy as jnp
import numpy as np
from jax import lax

D = 3584
HEADS = 16
KV_HEADS = 8
HD = 256
M = 32
SEGS = 2
TOKENS = 4096


def drawn_rows(row_key, row_count):
    return jnp.clip(jax.random.normal(jax.random.fold_in(row_key, 1), (row_count, D), jnp.float32), -6.0, 6.0)


def draw_segment_input(key, part):
    pieces = []
    for segment in range(SEGS):
        row_key = jax.random.fold_in(key, 500 + segment)
        pieces.append(drawn_rows(row_key, TOKENS))
    return jnp.stack(pieces, axis=0).astype(jnp.bfloat16)


def draw_memory(key, part):
    row_key = jax.random.fold_in(key, 700)
    result = drawn_rows(row_key, M)
    return result.astype(jnp.bfloat16)


def draw_w_query(key, part):
    weights = jnp.clip(jax.random.normal(jax.random.fold_in(key, 9201), (D, HEADS, HD), jnp.float32), -4.0, 4.0) * D ** (-0.5)
    return weights.reshape(D, HEADS * HD).astype(jnp.bfloat16)


def draw_w_key(key, part):
    weights = jnp.clip(jax.random.normal(jax.random.fold_in(key, 9202), (D, KV_HEADS, HD), jnp.float32), -4.0, 4.0) * D ** (-0.5)
    return weights.reshape(D, KV_HEADS * HD).astype(jnp.bfloat16)


def draw_mem_proj(key, part):
    weights = jnp.clip(jax.random.normal(jax.random.fold_in(key, 9203), (D, D), jnp.float32), -4.0, 4.0) * D ** (-0.5)
    return weights.astype(jnp.bfloat16)


def steps_of(own_key, dims, split, smallest, high):
    def one(dim, parts):
        steps = jax.random.uniform(jax.random.fold_in(jax.random.fold_in(own_key, 6), dim), (parts,), jnp.float32, smallest / len(split), high / len(split))
        return jnp.repeat(jnp.exp(steps), dims[dim] // parts).reshape((-1,) + (1,) * (len(dims) - dim - 1))

    loudness = one(*split[0])
    for cut in split[1:]:
        loudness = loudness * one(*cut)
    return loudness


def split_up(number_of, total, bound, lean):
    weights = [(1 << 20) // math.isqrt(rank ** lean) + 1 for rank in range(2, number_of + 1)]
    rest, counts = total - bound - (number_of - 1), [1] * (number_of - 1)
    while rest > 0:
        candidates = [i for i in range(number_of - 1) if counts[i] < bound]
        pool, budget = sum([weights[i] for i in candidates]), rest
        for i in candidates:
            extra = min(bound - counts[i], max(1, budget * weights[i] // pool), rest)
            counts[i] = counts[i] + extra
            rest = rest - extra
    return np.array([bound] + counts)


def ragged_sizes(rng, amount, total, most, slope):
    if amount == 2:
        one = jax.random.randint(rng, (), max(1, total - most), min(most, total - 1) + 1)
        return jnp.stack([one, total - one])
    sizes = jnp.asarray(split_up(amount, total, most, slope), jnp.int32)
    twos = (amount - 1) // 2
    source_of, taker = sizes[1:1 + 2 * twos:2], sizes[2:2 + 2 * twos:2]
    room = jnp.minimum(source_of - 1, most - taker)
    moved = jax.random.randint(jax.random.fold_in(rng, 1), (twos,), 0, 1 << 20) % (room + 1)
    sizes = sizes.at[1:1 + 2 * twos:2].set(source_of - moved).at[2:2 + 2 * twos:2].set(taker + moved)
    return sizes[jax.random.permutation(jax.random.fold_in(rng, 2), amount)]


def normal_values(own_key, extent, spread, limit, cuts=(), held_as=jnp.bfloat16):
    values = jax.random.normal(own_key, extent, jnp.float32) * spread
    if len(cuts) > 0:
        values = steps_of(own_key, extent, cuts, -0.22, 0.18) * values
    return jnp.clip(values, min=-limit, max=limit).astype(held_as)


def setup_inputs(seed: int = 0) -> dict:
    splits = jax.random.split(jax.random.key(seed), 10)
    return {
        "segment_input": draw_segment_input(jax.random.fold_in(splits[9], 71), 0),
        "doc_ids": jax.vmap(lambda own: jnp.searchsorted(jnp.cumsum(ragged_sizes(own, 4, TOKENS, TOKENS // 2, 0)), jnp.arange(TOKENS), side="right"))(jax.random.split(splits[1], SEGS)).reshape((SEGS, TOKENS)).astype(jnp.int32),
        "memory": draw_memory(jax.random.fold_in(splits[9], 71), 0),
        "gain": jnp.clip(1.0 + 0.18 * jax.random.normal(splits[3], (D,), jnp.float32), 0.099609375, 1.8984375).astype(jnp.bfloat16),
        "w_query": draw_w_query(jax.random.fold_in(splits[9], 71), 0),
        "w_key": draw_w_key(jax.random.fold_in(splits[9], 71), 0),
        "w_value": normal_values(splits[6], (D, KV_HEADS * HD), D ** -0.5, 0.09375, ((1, 8),)),
        "w_out": normal_values(splits[7], (HEADS * HD, D), (HEADS * HD) ** -0.5, 0.09375, ((1, 8),)),
        "mem_proj": draw_mem_proj(jax.random.fold_in(splits[9], 71), 0),
    }


def rms_norm(rows, gain):
    values = rows.astype(jnp.float32)
    scaled = values * lax.rsqrt(lax.optimization_barrier(jnp.mean(values * values, axis=-1, keepdims=True)) + 1e-06)
    return (scaled * gain.astype(jnp.float32)).astype(jnp.bfloat16)

def reference(segment_input, doc_ids, memory, gain, w_query, w_key, w_value, w_out, mem_proj):
    mem = memory
    outputs = []
    scale = jnp.float32(HD ** (-0.5))
    for seg in range(SEGS):
        tokens = segment_input[seg]
        docs = doc_ids[seg]
        normed_x = rms_norm(tokens, gain)
        normed_m = rms_norm(mem, gain)
        rows_all = jnp.concatenate([normed_x, normed_m], axis=0)
        query = jnp.dot(rows_all, w_query, preferred_element_type=jnp.float32).astype(jnp.bfloat16)
        keys = jnp.dot(rows_all, w_key, preferred_element_type=jnp.float32).astype(jnp.bfloat16)
        values = jnp.dot(rows_all, w_value, preferred_element_type=jnp.float32).astype(jnp.bfloat16)
        rows = TOKENS + M
        query = query.reshape(rows, KV_HEADS, 2, HD).transpose(1, 0, 2, 3)
        keys = jnp.concatenate([keys[TOKENS:], keys[:TOKENS]], axis=0).reshape(rows, KV_HEADS, HD).transpose(1, 0, 2)
        values = jnp.concatenate([values[TOKENS:], values[:TOKENS]], axis=0).reshape(rows, KV_HEADS, HD).transpose(1, 0, 2)
        position = jnp.arange(TOKENS, dtype=jnp.int32)
        allowed = (position[None, :] <= position[:, None]) & (docs[None, :] == docs[:, None])
        token_mask = jnp.concatenate([jnp.ones((TOKENS, M), dtype=bool), allowed], axis=1)
        mask = jnp.concatenate([token_mask, jnp.ones((M, rows), dtype=bool)], axis=0)

        def one_group(operands):
            group_query, group_keys, group_values = operands
            scores = jnp.einsum('rgd,kd->grk', group_query.astype(jnp.float32), group_keys.astype(jnp.float32)) * scale
            scores = jnp.where(mask[None], scores, -1e+30)
            peak = lax.optimization_barrier(jnp.max(scores, axis=-1, keepdims=True))
            weights = jnp.where(mask[None], jnp.exp(scores - peak), 0.0)
            total = lax.optimization_barrier(jnp.sum(weights, axis=-1))
            mixed = jnp.einsum('grk,kd->grd', weights.astype(jnp.bfloat16).astype(jnp.float32), group_values.astype(jnp.float32))
            return mixed / total[..., None]
        attended = lax.map(one_group, (query, keys, values))
        attended = attended.transpose(2, 0, 1, 3).reshape(rows, HEADS * HD).astype(jnp.bfloat16)
        attn_tok = attended[:TOKENS]
        attn_mem = attended[TOKENS:]
        outputs.append((tokens.astype(jnp.float32) + jnp.dot(attn_tok, w_out, preferred_element_type=jnp.float32)).astype(jnp.bfloat16))
        mem_out = (mem.astype(jnp.float32) + jnp.dot(attn_mem, w_out, preferred_element_type=jnp.float32)).astype(jnp.bfloat16)
        mem = jnp.dot(mem_out, mem_proj, preferred_element_type=jnp.float32).astype(jnp.bfloat16)
    return (jnp.stack(outputs, axis=0), mem)
```

```python
import math

import jax
import jax.numpy as jnp
from jax import lax
from jax.experimental import pallas as pl
from jax.experimental.pallas import tpu as pltpu
from jax.sharding import PartitionSpec as P

HD = 256
MESH = pl.DeviceIdType.MESH
F32 = jnp.float32
BF16 = jnp.bfloat16
NEG = -1e30
EXP_FACTOR = HD ** (-0.5) * math.log2(math.e)


def dot(a, b):
    return jnp.dot(a, b, preferred_element_type=F32)


def dot_t(a, b):
    return lax.dot_general(a, b, (((1,), (1,)), ((), ())), preferred_element_type=F32)


def body(
    x_hbm, docs_ref, mem_ref, gain_ref, wq_hbm, wk_hbm, wv_hbm, wo_hbm, mp_hbm,
    hid_ref, newmem_ref,
    xb, xr, wq, wk, wv, wo, mp, qb, kv, km, vm, nm, qmf, sc, mxs, lsum, acc, att, mg, pr, mb,
    load_sem, kv_send, kv_recv, att_send, att_recv, mg_send, mg_recv, pr_send, pr_recv, mb_send, mb_recv,
):
    segs, tok, width = x_hbm.shape
    s = lax.axis_index("seq")
    h = lax.axis_index("head")
    y, x = s // 4, s % 4
    z, c = h // 2, h % 2
    cols = wo_hbm.shape[1]

    loads = [
        pltpu.make_async_copy(x_hbm.at[0], xb.at[0], load_sem.at[0]),
        pltpu.make_async_copy(wk_hbm, wk, load_sem.at[1]),
        pltpu.make_async_copy(wv_hbm, wv, load_sem.at[2]),
        pltpu.make_async_copy(x_hbm.at[1], xb.at[1], load_sem.at[3]),
        pltpu.make_async_copy(wq_hbm, wq, load_sem.at[4]),
        pltpu.make_async_copy(
            mp_hbm.at[:, pl.ds(pl.multiple_of(y * 896, 128), 896)], mp, load_sem.at[5]),
        pltpu.make_async_copy(wo_hbm, wo, load_sem.at[6]),
        pltpu.make_async_copy(
            x_hbm.at[:, :, pl.ds(pl.multiple_of(z * 896, 128), 896)], xr, load_sem.at[7]),
    ]
    for one in loads:
        one.start()

    barrier = pltpu.get_barrier_semaphore()

    @pl.loop(1, 16)
    def _(p):
        pl.semaphore_signal(barrier, inc=1, device_id=((s + p) % 16, h), device_id_type=MESH)

    @pl.loop(1, 8)
    def _(p):
        pl.semaphore_signal(barrier, inc=1, device_id=(s, (h + p) % 8), device_id_type=MESH)

    def remote(src, dst, ssem, rsem, where):
        return pltpu.make_async_remote_copy(
            src_ref=src, dst_ref=dst, send_sem=ssem, recv_sem=rsem, device_id=where, device_id_type=MESH)

    sent = []

    def at(kind, i, j):
        dx, dy = (i, j) if kind == 0 else (j, i)
        return ((y + dy + 4) % 4) * 4 + (x + dx + 4) % 4

    def piece(kind, seg, i, j, half):
        ref = kv.at[kind, seg, at(kind, i, j)]
        return ref if half is None else ref.at[pl.ds(half * 128, 128)]

    counts = {}

    def kv_copy(kind, seg, i, j, half, di, dj):
        n = counts.get((kind, seg), 0)
        counts[(kind, seg)] = n + 1
        ref = piece(kind, seg, i, j, half)
        copy = remote(ref, ref, kv_send.at[kind, seg, n], kv_recv.at[kind, seg, at(kind, i, j), half or 0],
                      (at(kind, di, dj), h))
        copy.start()
        sent.append(copy)

    def kv_wait(kind, seg, i, j):
        halves = (0, 1) if (j == 2 or (i, j) == (2, 0)) else (None,)
        for half in halves:
            ref = piece(kind, seg, i, j, half)
            remote(ref, ref, kv_send.at[kind, seg, 0], kv_recv.at[kind, seg, at(kind, i, j), half or 0],
                   (at(kind, 1, 0), h)).wait_recv()

    def round0(seg):
        for kind in (0, 1):
            for di, dj in ((1, 0), (-1, 0), (0, 1), (0, -1)):
                kv_copy(kind, seg, 0, 0, None, di, dj)

    def round1(seg):
        for kind in (0, 1):
            kv_wait(kind, seg, -1, 0)
            kv_copy(kind, seg, -1, 0, 0, 1, 0)
            kv_copy(kind, seg, -1, 0, None, 0, 1)
            kv_copy(kind, seg, -1, 0, None, 0, -1)
            kv_wait(kind, seg, 1, 0)
            kv_copy(kind, seg, 1, 0, 1, -1, 0)
            kv_copy(kind, seg, 1, 0, None, 0, 1)
            kv_copy(kind, seg, 1, 0, None, 0, -1)
            kv_wait(kind, seg, 0, -1)
            kv_copy(kind, seg, 0, -1, 0, 0, 1)
            kv_wait(kind, seg, 0, 1)
            kv_copy(kind, seg, 0, 1, 1, 0, -1)

    def round2(seg):
        for kind in (0, 1):
            kv_wait(kind, seg, 2, 0)
            kv_copy(kind, seg, 2, 0, None, 0, 1)
            kv_copy(kind, seg, 2, 0, None, 0, -1)
            for i in (-1, 1):
                kv_wait(kind, seg, i, -1)
                kv_copy(kind, seg, i, -1, 0, 0, 1)
                kv_wait(kind, seg, i, 1)
                kv_copy(kind, seg, i, 1, 1, 0, -1)

    def round3(seg):
        for kind in (0, 1):
            kv_wait(kind, seg, 2, -1)
            kv_copy(kind, seg, 2, -1, 0, 0, 1)
            kv_wait(kind, seg, 2, 1)
            kv_copy(kind, seg, 2, 1, 1, 0, -1)

    def round4(seg):
        for kind in (0, 1):
            for i in (0, -1, 1, 2):
                kv_wait(kind, seg, i, 2)

    def head_at(dz, core):
        return ((z + dz + 4) % 4) * 2 + core

    def att_piece(seg, head, half):
        ref = att.at[seg, head]
        return ref if half is None else ref.at[pl.ds(half * 128, 128)]

    att_counts = {}

    def att_copy(seg, head, half, where):
        n = att_counts.get(seg, 0)
        att_counts[seg] = n + 1
        ref = att_piece(seg, head, half)
        copy = remote(ref, ref, att_send.at[seg, n], att_recv.at[seg, head, half or 0], (s, where))
        copy.start()
        sent.append(copy)

    def att_wait(seg, head, half=None):
        ref = att_piece(seg, head, half)
        remote(ref, ref, att_send.at[seg, 0], att_recv.at[seg, head, half or 0],
               (s, head_at(1, c))).wait_recv()

    other = 1 - c

    def heads0(seg):
        att_copy(seg, h, None, head_at(1, c))
        att_copy(seg, h, None, head_at(-1, c))
        att_copy(seg, h, None, head_at(0, other))

    def heads1(seg):
        att_wait(seg, head_at(-1, c))
        att_copy(seg, head_at(-1, c), 0, head_at(1, c))
        att_copy(seg, head_at(-1, c), None, head_at(0, other))
        att_wait(seg, head_at(1, c))
        att_copy(seg, head_at(1, c), 1, head_at(-1, c))
        att_copy(seg, head_at(1, c), None, head_at(0, other))

    def heads2(seg):
        att_wait(seg, head_at(2, c), 0)
        att_wait(seg, head_at(2, c), 1)
        att_copy(seg, head_at(2, c), None, head_at(0, other))

    def heads3(seg):
        for dz in (0, -1, 1, 2):
            att_wait(seg, head_at(dz, other))

    def to_heads(ref, ssem, rsem, seg):
        @pl.loop(1, 8)
        def _(p):
            remote(ref.at[seg, h], ref.at[seg, h], ssem.at[seg, p], rsem.at[seg, h], (s, (h + p) % 8)).start()

    def from_heads(ref, ssem, rsem, seg):
        @pl.loop(1, 8)
        def _(p):
            who = (h + p) % 8
            remote(ref.at[seg, who], ref.at[seg, who], ssem.at[seg, p], rsem.at[seg, who], (s, who)).wait_recv()

    def sent_heads(ref, ssem, rsem, seg):
        @pl.loop(1, 8)
        def _(p):
            remote(ref.at[seg, h], ref.at[seg, h], ssem.at[seg, p], rsem.at[seg, h], (s, (h + p) % 8)).wait_send()

    def to_seq(seg):
        @pl.loop(1, 16)
        def _(p):
            remote(mb.at[seg + 1, s], mb.at[seg + 1, s], mb_send.at[seg, p], mb_recv.at[seg, s],
                   ((s + p) % 16, h)).start()

    def from_seq(seg):
        @pl.loop(1, 16)
        def _(p):
            who = (s + p) % 16
            remote(mb.at[seg + 1, who], mb.at[seg + 1, who], mb_send.at[seg, p], mb_recv.at[seg, who],
                   (who, h)).wait_recv()

    def sent_seq(seg):
        @pl.loop(1, 16)
        def _(p):
            remote(mb.at[seg + 1, s], mb.at[seg + 1, s], mb_send.at[seg, p], mb_recv.at[seg, s],
                   ((s + p) % 16, h)).wait_send()

    gain = gain_ref[...].astype(F32)

    def norm_tokens(seg):
        @pl.loop(0, tok // 16)
        def _(i):
            rows = pl.ds(pl.multiple_of(i * 16, 16), 16)
            v = xb[seg, rows, :].astype(F32)
            mean = jnp.sum(v * v, axis=-1, keepdims=True) * (1.0 / width)
            xb[seg, rows, :] = (v * lax.rsqrt(mean + 1e-06) * gain).astype(BF16)

    def keys_values(seg):
        kv[0, seg, s] = dot(xb[seg], wk[...]).astype(BF16)
        kv[1, seg, s] = dot(xb[seg], wv[...]).astype(BF16)

    def memory_rows(version, pair):
        rows = []
        for xx in (2 * pair, 2 * pair + 1):
            rows.append(jnp.concatenate([mb[version, yy * 4 + xx] for yy in range(4)], axis=1))
        return jnp.concatenate(rows, axis=0)

    def project_memory(version):
        for pair in range(2):
            v = memory_rows(version, pair)
            mean = jnp.sum(v * v, axis=-1, keepdims=True) * (1.0 / width)
            nm[pair * 16:pair * 16 + 16, :] = (v * lax.rsqrt(mean + 1e-06) * gain).astype(BF16)
        km[0:32, :] = dot(nm[...], wk[...]).astype(BF16)
        vm[0:32, :] = dot(nm[...], wv[...]).astype(BF16)
        qmf[...] = dot(nm[...], wq[...]).astype(BF16).astype(F32)

    def weights_of(scores, peak):
        return jnp.exp2((scores - peak) * EXP_FACTOR)

    def memory_scores(q):
        lane = lax.broadcasted_iota(jnp.int32, (q.shape[0], 128), 1)
        return jnp.where(lane < 32, dot_t(q, km[...]), NEG)

    def attend_memory(seg):
        own = pl.ds(pl.multiple_of(x * 8, 8), 8)
        q = jnp.concatenate([qmf[own, 0:256], qmf[own, 256:512]], axis=0).astype(BF16)
        keys = kv[0, seg].reshape(16 * tok, HD)
        values = kv[1, seg].reshape(16 * tok, HD)
        first = memory_scores(q)
        scores = dot_t(q, keys)
        peak = jnp.maximum(jnp.max(first, axis=1, keepdims=True), jnp.max(scores, axis=1, keepdims=True))
        w_first = weights_of(first, peak)
        w = weights_of(scores, peak)
        total = jnp.sum(w_first, axis=1, keepdims=True) + jnp.sum(w, axis=1, keepdims=True)
        mixed = dot(w_first.astype(BF16), vm[...]) + dot(w.astype(BF16), values)
        result = (mixed / total).astype(BF16)
        mg[seg, h, :, 0:256] = result[0:8]
        mg[seg, h, :, 256:512] = result[8:16]

    def write_memory(seg):
        out = dot(mg[seg, 0], wo[0:512, :])
        for head in range(1, 8):
            out = out + dot(mg[seg, head], wo[head * 512:head * 512 + 512, :])
        old = mb[seg, z * 4 + x]
        old = jnp.where(c == 0, old[:, 0:cols], old[:, cols:2 * cols])
        mem_out = (old + out).astype(BF16)
        pr[seg, h] = dot(mem_out, mp[...])

    def sum_memory(seg):
        total = pr[seg, 0]
        for head in range(1, 8):
            total = total + pr[seg, head]
        mb[seg + 1, s] = total.astype(BF16).astype(F32)

    def attend(seg, g):
        lanes = pl.ds(g * HD, HD)
        docs = docs_ref[seg:seg + 1, :]
        pos = s * tok + lax.broadcasted_iota(jnp.int32, (tok, 1), 0)
        start = jnp.zeros((tok, 1), jnp.int32)
        for doc in (1, 2, 3):
            begin = jnp.sum(jnp.where(docs < doc, 1, 0), axis=1, keepdims=True)
            start = jnp.maximum(start, jnp.where(begin <= pos, begin, 0))
        reach = jnp.minimum(s, 8) + 1
        mxs[...] = memory_scores(qb[seg, :, lanes])

        @pl.loop(0, reach)
        def _(d):
            t = s - d
            scores = dot_t(qb[seg, :, lanes], kv[0, seg, t])
            key_pos = t * tok + lax.broadcasted_iota(jnp.int32, (tok, tok), 1)
            scores = jnp.where((key_pos >= start) & (key_pos <= pos), scores, NEG)
            sc[d] = scores
            mxs[...] = jnp.maximum(mxs[...], jnp.maximum(scores[:, 0:128], scores[:, 128:256]))

        peak = jnp.max(mxs[...], axis=1, keepdims=True)
        w_first = weights_of(memory_scores(qb[seg, :, lanes]), peak)
        lsum[...] = w_first
        acc[...] = dot(w_first.astype(BF16), vm[...])

        @pl.loop(0, reach)
        def _(d):
            w = weights_of(sc[d], peak)
            lsum[...] += w[:, 0:128] + w[:, 128:256]
            acc[...] += dot(w.astype(BF16), kv[1, seg, s - d])

        total = jnp.sum(lsum[...], axis=1, keepdims=True)
        att[seg, h, :, lanes] = (acc[...] / total).astype(BF16)

    def project_tokens(seg):
        out = dot(att[seg, 0], wo[0:512, :])
        for head in range(1, 8):
            out = out + dot(att[seg, head], wo[head * 512:head * 512 + 512, :])
        old = xr[seg].astype(F32)
        old = jnp.where(c == 0, old[:, 0:cols], old[:, cols:2 * cols])
        hid_ref[seg] = (old + out).astype(BF16)

    for xx in range(4):
        for yy in range(4):
            mb[0, yy * 4 + xx] = mem_ref[8 * xx:8 * xx + 8, 896 * yy:896 * yy + 896].astype(F32)
    km[...] = jnp.zeros_like(km)
    vm[...] = jnp.zeros_like(vm)
    loads[0].wait()
    norm_tokens(0)
    loads[1].wait()
    loads[2].wait()
    keys_values(0)
    pl.semaphore_wait(barrier, 22)
    round0(0)
    loads[3].wait()
    norm_tokens(1)
    keys_values(1)
    loads[4].wait()
    project_memory(0)
    qb[0] = dot(xb[0], wq[...]).astype(BF16)
    round1(0)
    round0(1)
    qb[1] = dot(xb[1], wq[...]).astype(BF16)
    round2(0)
    round1(1)
    round3(0)
    round4(0)
    for k in (5, 6, 7):
        loads[k].wait()

    attend_memory(0)
    to_heads(mg, mg_send, mg_recv, 0)
    attend(0, 0)
    attend(0, 1)
    heads0(0)
    from_heads(mg, mg_send, mg_recv, 0)
    write_memory(0)
    to_heads(pr, pr_send, pr_recv, 0)
    round2(1)
    heads1(0)
    from_heads(pr, pr_send, pr_recv, 0)
    sum_memory(0)
    to_seq(0)
    round3(1)
    heads2(0)
    from_seq(0)
    project_memory(1)
    heads3(0)
    project_tokens(0)
    round4(1)

    attend_memory(1)
    to_heads(mg, mg_send, mg_recv, 1)
    attend(1, 0)
    attend(1, 1)
    heads0(1)
    from_heads(mg, mg_send, mg_recv, 1)
    write_memory(1)
    to_heads(pr, pr_send, pr_recv, 1)
    heads1(1)
    from_heads(pr, pr_send, pr_recv, 1)
    sum_memory(1)
    to_seq(1)
    heads2(1)
    from_seq(1)
    for pair in range(2):
        newmem_ref[pair * 16:pair * 16 + 16, :] = memory_rows(2, pair).astype(BF16)
    heads3(1)
    project_tokens(1)

    for copy in sent:
        copy.wait_send()
    for seg in range(2):
        sent_heads(mg, mg_send, mg_recv, seg)
        sent_heads(pr, pr_send, pr_recv, seg)
        sent_seq(seg)


def per_device(segment_input, doc_ids, memory, gain, w_query, w_key, w_value, w_out, mem_proj):
    segs, tok, width = segment_input.shape
    cols = w_out.shape[1]
    anywhere = pl.BlockSpec(memory_space=pl.ANY)
    vmem = pl.BlockSpec(memory_space=pltpu.VMEM)
    dma = pltpu.SemaphoreType.DMA
    return pl.pallas_call(
        body,
        out_shape=(
            jax.ShapeDtypeStruct((segs, tok, cols), BF16),
            jax.ShapeDtypeStruct(memory.shape, BF16),
        ),
        in_specs=[anywhere, vmem, vmem, vmem, anywhere, anywhere, anywhere, anywhere, anywhere],
        out_specs=(vmem, vmem),
        scratch_shapes=[
            pltpu.VMEM((segs, tok, width), BF16),
            pltpu.VMEM((segs, tok, 896), BF16),
            pltpu.VMEM(w_query.shape, BF16),
            pltpu.VMEM(w_key.shape, BF16),
            pltpu.VMEM(w_value.shape, BF16),
            pltpu.VMEM(w_out.shape, BF16),
            pltpu.VMEM((mem_proj.shape[0], 896), BF16),
            pltpu.VMEM((segs, tok, 2 * HD), BF16),
            pltpu.VMEM((2, segs, 16, tok, HD), BF16),
            pltpu.VMEM((128, HD), BF16),
            pltpu.VMEM((128, HD), BF16),
            pltpu.VMEM((32, width), BF16),
            pltpu.VMEM((32, 2 * HD), F32),
            pltpu.VMEM((9, tok, tok), F32),
            pltpu.VMEM((tok, 128), F32),
            pltpu.VMEM((tok, 128), F32),
            pltpu.VMEM((tok, HD), F32),
            pltpu.VMEM((segs, 8, tok, 2 * HD), BF16),
            pltpu.VMEM((segs, 8, 8, 2 * HD), BF16),
            pltpu.VMEM((segs, 8, 8, 896), F32),
            pltpu.VMEM((segs + 1, 16, 8, 896), F32),
            dma((8,)),
            dma((2, segs, 20)),
            dma((2, segs, 16, 2)),
            dma((segs, 8)),
            dma((segs, 8, 2)),
            dma((segs, 8)),
            dma((segs, 8)),
            dma((segs, 8)),
            dma((segs, 8)),
            dma((segs, 16)),
            dma((segs, 16)),
        ],
        compiler_params=pltpu.CompilerParams(
            collective_id=0, has_side_effects=True, vmem_limit_bytes=60000 * 1024),
    )(segment_input, doc_ids, memory, gain.reshape(1, -1), w_query, w_key, w_value, w_out, mem_proj)


def solution(mesh):
    return jax.shard_map(
        per_device,
        mesh=mesh,
        in_specs=(
            P(None, "seq", None),
            P(),
            P(),
            P(),
            P(None, "head"),
            P(None, "head"),
            P(None, "head"),
            P(None, "head"),
            P("head", None),
        ),
        out_specs=(P(None, "seq", "head"), P()),
        check_vma=False,
    )
```

```python
import math

import jax
import jax.numpy as jnp
from jax import lax
from jax.experimental import pallas as pl
from jax.experimental.pallas import tpu as pltpu
from jax.sharding import PartitionSpec as P

HD = 256
MESH = pl.DeviceIdType.MESH
F32 = jnp.float32
BF16 = jnp.bfloat16
NEG = -1e30
EXP_FACTOR = HD ** (-0.5) * math.log2(math.e)


def scoped(f):
    def g(*args):
        with jax.named_scope(f.__name__ + "".join(f"_{a}" for a in args if isinstance(a, int))):
            return f(*args)
    return g


def dot(a, b):
    return jnp.dot(a, b, preferred_element_type=F32)


def dot_t(a, b):
    return lax.dot_general(a, b, (((1,), (1,)), ((), ())), preferred_element_type=F32)


def body(
    x_hbm, docs_ref, mem_ref, gain_ref, wq_hbm, wk_hbm, wv_hbm, wo_hbm, mp_hbm,
    hid_ref, newmem_ref,
    xb, xr, xt, wq, wk, wv, wo, mp, qb, kv, km, vm, nm, memb, qm, sc, mxs, lsum, acc, att, ps, po, mg, pr, mb,
    load_sem, kv_send, kv_recv, att_send, att_recv, ps_send, po_recv, mg_send, mg_recv, pr_send, pr_recv, mb_send, mb_recv,
):
    segs, tok, width = x_hbm.shape
    s = lax.axis_index("seq")
    h = lax.axis_index("head")
    y, x = s // 4, s % 4
    z, c = h // 2, h % 2
    cols = wo_hbm.shape[0]

    loads = [
        pltpu.make_async_copy(x_hbm.at[0], xb.at[0], load_sem.at[0]),
        pltpu.make_async_copy(wk_hbm, wk, load_sem.at[1]),
        pltpu.make_async_copy(wv_hbm, wv, load_sem.at[2]),
        pltpu.make_async_copy(x_hbm.at[1], xb.at[1], load_sem.at[3]),
        pltpu.make_async_copy(wq_hbm, wq, load_sem.at[4]),
        pltpu.make_async_copy(mp_hbm, mp, load_sem.at[5]),
        pltpu.make_async_copy(wo_hbm, wo, load_sem.at[6]),
        pltpu.make_async_copy(
            x_hbm.at[:, :, pl.ds(pl.multiple_of(z * 896, 128), 896)], xr, load_sem.at[7]),
    ]
    for one in loads:
        one.start()

    barrier = pltpu.get_barrier_semaphore()

    @pl.loop(1, 16)
    def _(p):
        pl.semaphore_signal(barrier, inc=1, device_id=((s + p) % 16, h), device_id_type=MESH)

    @pl.loop(1, 8)
    def _(p):
        pl.semaphore_signal(barrier, inc=1, device_id=(s, (h + p) % 8), device_id_type=MESH)

    def remote(src, dst, ssem, rsem, where):
        return pltpu.make_async_remote_copy(
            src_ref=src, dst_ref=dst, send_sem=ssem, recv_sem=rsem, device_id=where, device_id_type=MESH)

    sent = []

    def at(kind, i, j):
        dx, dy = (i, j) if kind == 0 else (j, i)
        return ((y + dy + 4) % 4) * 4 + (x + dx + 4) % 4

    def piece(kind, seg, i, j, half):
        ref = kv.at[kind, seg, at(kind, i, j)]
        return ref if half is None else ref.at[pl.ds(half * 128, 128)]

    counts = {}

    def kv_copy(kind, seg, i, j, half, di, dj):
        n = counts.get((kind, seg), 0)
        counts[(kind, seg)] = n + 1
        ref = piece(kind, seg, i, j, half)
        copy = remote(ref, ref, kv_send.at[kind, seg, n], kv_recv.at[kind, seg, at(kind, i, j), half or 0],
                      (at(kind, di, dj), h))
        copy.start()
        sent.append(copy)

    def kv_wait(kind, seg, i, j):
        halves = (0, 1) if (j == 2 or (i, j) == (2, 0)) else (None,)
        for half in halves:
            ref = piece(kind, seg, i, j, half)
            remote(ref, ref, kv_send.at[kind, seg, 0], kv_recv.at[kind, seg, at(kind, i, j), half or 0],
                   (at(kind, 1, 0), h)).wait_recv()

    @scoped
    def round0(seg):
        for kind in (0, 1):
            for di, dj in ((1, 0), (-1, 0), (0, 1), (0, -1)):
                kv_copy(kind, seg, 0, 0, None, di, dj)

    @scoped
    def round1(seg):
        for kind in (0, 1):
            kv_wait(kind, seg, -1, 0)
            kv_copy(kind, seg, -1, 0, 0, 1, 0)
            kv_copy(kind, seg, -1, 0, None, 0, 1)
            kv_copy(kind, seg, -1, 0, None, 0, -1)
            kv_wait(kind, seg, 1, 0)
            kv_copy(kind, seg, 1, 0, 1, -1, 0)
            kv_copy(kind, seg, 1, 0, None, 0, 1)
            kv_copy(kind, seg, 1, 0, None, 0, -1)
            kv_wait(kind, seg, 0, -1)
            kv_copy(kind, seg, 0, -1, 0, 0, 1)
            kv_wait(kind, seg, 0, 1)
            kv_copy(kind, seg, 0, 1, 1, 0, -1)

    @scoped
    def round2(seg):
        for kind in (0, 1):
            kv_wait(kind, seg, 2, 0)
            kv_copy(kind, seg, 2, 0, None, 0, 1)
            kv_copy(kind, seg, 2, 0, None, 0, -1)
            for i in (-1, 1):
                kv_wait(kind, seg, i, -1)
                kv_copy(kind, seg, i, -1, 0, 0, 1)
                kv_wait(kind, seg, i, 1)
                kv_copy(kind, seg, i, 1, 1, 0, -1)

    @scoped
    def round3(seg):
        for kind in (0, 1):
            kv_wait(kind, seg, 2, -1)
            kv_copy(kind, seg, 2, -1, 0, 0, 1)
            kv_wait(kind, seg, 2, 1)
            kv_copy(kind, seg, 2, 1, 1, 0, -1)

    @scoped
    def round4(seg):
        for kind in (0, 1):
            for i in (0, -1, 1, 2):
                kv_wait(kind, seg, i, 2)

    def head_at(dz, core):
        return ((z + dz + 4) % 4) * 2 + core

    def att_piece(seg, head, half):
        ref = att.at[seg, head]
        return ref if half is None else ref.at[pl.ds(half * 128, 128)]

    att_counts = {}

    def att_copy(seg, head, half, where):
        n = att_counts.get(seg, 0)
        att_counts[seg] = n + 1
        ref = att_piece(seg, head, half)
        copy = remote(ref, ref, att_send.at[seg, n], att_recv.at[seg, head, half or 0], (s, where))
        copy.start()
        sent.append(copy)

    def att_wait(seg, head, half=None):
        ref = att_piece(seg, head, half)
        remote(ref, ref, att_send.at[seg, 0], att_recv.at[seg, head, half or 0],
               (s, head_at(1, c))).wait_recv()

    other = 1 - c

    @scoped
    def heads0(seg):
        att_copy(seg, h, None, head_at(1, c))
        att_copy(seg, h, None, head_at(-1, c))
        att_copy(seg, h, None, head_at(0, other))

    @scoped
    def heads1(seg):
        att_wait(seg, head_at(-1, c))
        att_copy(seg, head_at(-1, c), 0, head_at(1, c))
        att_copy(seg, head_at(-1, c), None, head_at(0, other))
        att_wait(seg, head_at(1, c))
        att_copy(seg, head_at(1, c), 1, head_at(-1, c))
        att_copy(seg, head_at(1, c), None, head_at(0, other))

    @scoped
    def heads2(seg):
        att_wait(seg, head_at(2, c), 0)
        att_wait(seg, head_at(2, c), 1)
        att_copy(seg, head_at(2, c), None, head_at(0, other))

    @scoped
    def heads3(seg):
        for dz in (0, -1, 1, 2):
            att_wait(seg, head_at(dz, other))

    def to_owners(seg):
        @pl.loop(1, 16)
        def _(p):
            who = (s + p) % 16
            remote(ps.at[seg, who], po.at[seg, s], ps_send.at[seg, p], po_recv.at[seg, s], (who, h)).start()

    @scoped
    def from_owners(seg):
        @pl.loop(1, 16)
        def _(p):
            who = (s + p) % 16
            remote(po.at[seg, who], po.at[seg, who], ps_send.at[seg, p], po_recv.at[seg, who], (who, h)).wait_recv()

    def sent_owners(seg):
        @pl.loop(1, 16)
        def _(p):
            who = (s + p) % 16
            remote(ps.at[seg, who], po.at[seg, s], ps_send.at[seg, p], po_recv.at[seg, s], (who, h)).wait_send()

    def to_heads(ref, ssem, rsem, seg):
        @pl.loop(1, 8)
        def _(p):
            remote(ref.at[seg, h], ref.at[seg, h], ssem.at[seg, p], rsem.at[seg, h], (s, (h + p) % 8)).start()

    @scoped
    def from_heads(ref, ssem, rsem, seg):
        @pl.loop(1, 8)
        def _(p):
            who = (h + p) % 8
            remote(ref.at[seg, who], ref.at[seg, who], ssem.at[seg, p], rsem.at[seg, who], (s, who)).wait_recv()

    def sent_heads(ref, ssem, rsem, seg):
        @pl.loop(1, 8)
        def _(p):
            remote(ref.at[seg, h], ref.at[seg, h], ssem.at[seg, p], rsem.at[seg, h], (s, (h + p) % 8)).wait_send()

    def to_seq(seg):
        @pl.loop(1, 16)
        def _(p):
            remote(mb.at[seg, s], mb.at[seg, s], mb_send.at[seg, p], mb_recv.at[seg, s],
                   ((s + p) % 16, h)).start()

    @scoped
    def from_seq(seg):
        @pl.loop(1, 16)
        def _(p):
            who = (s + p) % 16
            remote(mb.at[seg, who], mb.at[seg, who], mb_send.at[seg, p], mb_recv.at[seg, who],
                   (who, h)).wait_recv()

    def sent_seq(seg):
        @pl.loop(1, 16)
        def _(p):
            remote(mb.at[seg, s], mb.at[seg, s], mb_send.at[seg, p], mb_recv.at[seg, s],
                   ((s + p) % 16, h)).wait_send()

    gain = gain_ref[...].astype(F32).reshape(1, width)

    @scoped
    def norm_tokens(seg):
        @pl.loop(0, tok // 16)
        def _(i):
            rows = pl.ds(pl.multiple_of(i * 16, 16), 16)
            v = xb[seg, rows, :].astype(F32)
            mean = jnp.sum(v * v, axis=-1, keepdims=True) * (1.0 / width)
            xb[seg, rows, :] = (v * lax.rsqrt(mean + 1e-06) * gain).astype(BF16)

    @scoped
    def keys_values(seg):
        kv[0, seg, s] = dot(xb[seg], wk[...]).astype(BF16)
        kv[1, seg, s] = dot(xb[seg], wv[...]).astype(BF16)

    @scoped
    def gather_memory(seg):
        blocks = mb[seg].reshape(128, 896)
        m = lax.broadcasted_iota(jnp.int32, (32, 128), 0)
        j = lax.broadcasted_iota(jnp.int32, (32, 128), 1)
        for yy in range(4):
            pick = (m == (j // 8) * 2 + j % 2) & ((j % 8) // 2 == yy)
            memb[:, 896 * yy:896 * yy + 896] = dot(jnp.where(pick, 1.0, 0.0).astype(BF16), blocks).astype(BF16)

    @scoped
    def project_memory(seg):
        for pair in range(2):
            v = memb[pair * 16:pair * 16 + 16, :].astype(F32)
            mean = jnp.sum(v * v, axis=-1, keepdims=True) * (1.0 / width)
            nm[pair * 16:pair * 16 + 16, :] = (v * lax.rsqrt(mean + 1e-06) * gain).astype(BF16)
        qm[...] = dot(nm[...], wq[...]).astype(BF16)
        km[seg, 0:32, :] = dot(nm[...], wk[...]).astype(BF16)
        vm[seg, 0:32, :] = dot(nm[...], wv[...]).astype(BF16)

    def weights_of(scores, peak):
        return jnp.exp2((scores - peak) * EXP_FACTOR)

    def memory_scores(q, seg):
        lane = lax.broadcasted_iota(jnp.int32, (q.shape[0], 128), 1)
        return jnp.where(lane < 32, dot_t(q, km[seg]), NEG)

    @scoped
    def attend_memory(seg):
        q = jnp.concatenate([qm[:, 0:256], qm[:, 256:512]], axis=0)
        lane = lax.broadcasted_iota(jnp.int32, (64, 128), 1)
        first = jnp.where((lane < 32) & (s == 0), dot_t(q, km[seg]), NEG)
        scores = dot_t(q, kv[0, seg, s])
        peak = jnp.maximum(jnp.max(first, axis=1, keepdims=True), jnp.max(scores, axis=1, keepdims=True))
        w_first = weights_of(first, peak)
        w = weights_of(scores, peak)
        total = jnp.sum(w_first, axis=1, keepdims=True) + jnp.sum(w, axis=1, keepdims=True)
        mixed = dot(w_first.astype(BF16), vm[seg]) + dot(w.astype(BF16), kv[1, seg, s])
        stats = jnp.where(lane < 64, peak, total)
        for t in range(16):
            for g in range(2):
                row = 32 * g + 2 * t
                ps[seg, t, 2 * g:2 * g + 2, 0:256] = mixed[row:row + 2]
                ps[seg, t, 2 * g:2 * g + 2, 256:384] = stats[row:row + 2]
        po[seg, s] = ps[seg, s]

    @scoped
    def combine_memory(seg):
        peaks = [po[seg, t, :, 256:257] for t in range(16)]
        peak = peaks[0]
        for one in peaks[1:]:
            peak = jnp.maximum(peak, one)
        total = jnp.zeros((4, 1), F32)
        mixed = jnp.zeros((4, 256), F32)
        for t in range(16):
            f = weights_of(peaks[t], peak)
            total = total + f * po[seg, t, :, 320:321]
            mixed = mixed + f * po[seg, t, :, 0:256]
        result = mixed / total
        for g in range(2):
            mg[seg, h, :, 256 * g:256 * g + 256] = jnp.concatenate([result[2 * g:2 * g + 2]] * 4, axis=0).astype(BF16)

    @scoped
    def write_memory(seg):
        out = dot_t(mg[seg, 0], wo[:, 0:512])
        for head in range(1, 8):
            out = out + dot_t(mg[seg, head], wo[:, head * 512:head * 512 + 512])
        k = lax.broadcasted_iota(jnp.int32, (8, 32), 0)
        m = lax.broadcasted_iota(jnp.int32, (8, 32), 1)
        own = jnp.where(m == 2 * s + k % 2, 1.0, 0.0).astype(BF16)
        old = dot(own, memb[:, pl.ds(pl.multiple_of(z * 896, 128), 896)])
        old = jnp.where(c == 0, old[:, 0:cols], old[:, cols:2 * cols])
        part = dot((old + out).astype(BF16), mp[...])
        k = lax.broadcasted_iota(jnp.int32, (8, 896), 0)
        block = part[:, 0:896]
        for yy in range(1, 4):
            block = jnp.where(k // 2 == yy, part[:, 896 * yy:896 * yy + 896], block)
        pr[seg, h] = block.astype(BF16)

    @scoped
    def sum_memory(seg):
        total = pr[seg, 0].astype(F32)
        for head in range(1, 8):
            total = total + pr[seg, head].astype(F32)
        mb[seg, s] = total.astype(BF16)

    def first_keys(seg):
        docs = docs_ref[seg:seg + 1, :]
        pos = s * tok + lax.broadcasted_iota(jnp.int32, (tok, 1), 0)
        start = jnp.zeros((tok, 1), jnp.int32)
        for doc in (1, 2, 3):
            begin = jnp.sum(jnp.where(docs < doc, 1, 0), axis=1, keepdims=True)
            start = jnp.maximum(start, jnp.where(begin <= pos, begin, 0))
        return start, pos

    def score_blocks(seg, low, high):
        start, pos = first_keys(seg)

        @pl.loop(low, high)
        def _(d):
            t = s - d
            key_pos = t * tok + lax.broadcasted_iota(jnp.int32, (tok, tok), 1)
            ok = (key_pos >= start) & (key_pos <= pos)
            for g in range(2):
                scores = jnp.where(ok, dot_t(qb[seg, :, g * HD:g * HD + HD], kv[0, seg, t]), NEG)
                sc[g, d] = scores
                mxs[g] = jnp.maximum(mxs[g], jnp.maximum(scores[:, 0:128], scores[:, 128:256]))

    near = jnp.minimum(s, x + 4) + 1
    reach = jnp.minimum(s, 8) + 1

    @scoped
    def scores_near(seg):
        mxs[...] = jnp.full_like(mxs, NEG)
        score_blocks(seg, 0, near)

    @scoped
    def scores_far(seg):
        score_blocks(seg, near, reach)

    @scoped
    def attend(seg):
        peaks = []
        for g in range(2):
            first = memory_scores(qb[seg, :, g * HD:g * HD + HD], seg)
            peak = jnp.max(jnp.maximum(mxs[g], first), axis=1, keepdims=True)
            w_first = weights_of(first, peak)
            lsum[g] = w_first
            acc[g] = dot(w_first.astype(BF16), vm[seg])
            peaks.append(peak)

        @pl.loop(0, reach)
        def _(d):
            for g in range(2):
                w = weights_of(sc[g, d], peaks[g])
                lsum[g] += w[:, 0:128] + w[:, 128:256]
                acc[g] += dot(w.astype(BF16), kv[1, seg, s - d])

        for g in range(2):
            total = jnp.sum(lsum[g], axis=1, keepdims=True)
            att[seg, h, :, g * HD:g * HD + HD] = (acc[g] / total).astype(BF16)

    @scoped
    def project_tokens(seg):
        out = dot_t(wo[:, 0:512], att[seg, 0])
        for head in range(1, 8):
            out = out + dot_t(wo[:, head * 512:head * 512 + 512], att[seg, head])
        hid_ref[seg] = (xt[seg] + out).astype(BF16)

    @scoped
    def residual(seg):
        old = xr[seg].astype(F32).T
        xt[seg] = jnp.where(c == 0, old[0:cols], old[cols:2 * cols])

    memb[...] = mem_ref[...]
    km[...] = jnp.zeros_like(km)
    vm[...] = jnp.zeros_like(vm)
    with jax.named_scope("load0"):
        loads[0].wait()
    norm_tokens(0)
    with jax.named_scope("load1"):
        loads[1].wait()
        loads[2].wait()
    keys_values(0)
    with jax.named_scope("barrier"):
        pl.semaphore_wait(barrier, 22)
    round0(0)
    with jax.named_scope("load4"):
        loads[4].wait()
    project_memory(0)
    attend_memory(0)
    to_owners(0)
    with jax.named_scope("load3"):
        loads[3].wait()
    norm_tokens(1)
    keys_values(1)
    round1(0)
    round0(1)
    with jax.named_scope("query"):
        qb[0] = dot(xb[0], wq[...]).astype(BF16)
    from_owners(0)
    combine_memory(0)
    to_heads(mg, mg_send, mg_recv, 0)
    with jax.named_scope("query"):
        qb[1] = dot(xb[1], wq[...]).astype(BF16)
    for k in (5, 6, 7):
        loads[k].wait()
    from_heads(mg, mg_send, mg_recv, 0)
    write_memory(0)
    to_heads(pr, pr_send, pr_recv, 0)
    round2(0)
    from_heads(pr, pr_send, pr_recv, 0)
    sum_memory(0)
    to_seq(0)
    round1(1)
    from_seq(0)
    gather_memory(0)
    project_memory(1)
    attend_memory(1)
    to_owners(1)
    round3(0)
    scores_near(0)
    round2(1)
    residual(0)
    residual(1)
    from_owners(1)
    combine_memory(1)
    to_heads(mg, mg_send, mg_recv, 1)
    round4(0)
    scores_far(0)
    attend(0)
    from_heads(mg, mg_send, mg_recv, 1)
    write_memory(1)
    to_heads(pr, pr_send, pr_recv, 1)
    heads0(0)
    round3(1)
    from_heads(pr, pr_send, pr_recv, 1)
    sum_memory(1)
    to_seq(1)
    heads1(0)
    scores_near(1)
    heads2(0)
    round4(1)
    scores_far(1)
    attend(1)
    heads0(1)
    heads3(0)
    project_tokens(0)
    from_seq(1)
    gather_memory(1)
    newmem_ref[...] = memb[...]
    heads1(1)
    heads2(1)
    heads3(1)
    project_tokens(1)

    for copy in sent:
        copy.wait_send()
    for seg in range(2):
        sent_heads(mg, mg_send, mg_recv, seg)
        sent_heads(pr, pr_send, pr_recv, seg)
        sent_seq(seg)
        sent_owners(seg)


def per_device(segment_input, doc_ids, memory, gain, w_query, w_key, w_value, w_out, mem_proj):
    segs, tok, width = segment_input.shape
    cols = w_out.shape[1]
    anywhere = pl.BlockSpec(memory_space=pl.ANY)
    vmem = pl.BlockSpec(memory_space=pltpu.VMEM)
    dma = pltpu.SemaphoreType.DMA
    hidden_t, new_memory = pl.pallas_call(
        body,
        out_shape=(
            jax.ShapeDtypeStruct((segs, cols, tok), BF16),
            jax.ShapeDtypeStruct(memory.shape, BF16),
        ),
        in_specs=[anywhere, vmem, vmem, vmem, anywhere, anywhere, anywhere, anywhere, anywhere],
        out_specs=(vmem, vmem),
        scratch_shapes=[
            pltpu.VMEM((segs, tok, width), BF16),
            pltpu.VMEM((segs, tok, 896), BF16),
            pltpu.VMEM((segs, cols, tok), F32),
            pltpu.VMEM(w_query.shape, BF16),
            pltpu.VMEM(w_key.shape, BF16),
            pltpu.VMEM(w_value.shape, BF16),
            pltpu.VMEM((cols, w_out.shape[0]), BF16),
            pltpu.VMEM(mem_proj.shape, BF16),
            pltpu.VMEM((segs, tok, 2 * HD), BF16),
            pltpu.VMEM((2, segs, 16, tok, HD), BF16),
            pltpu.VMEM((segs, 128, HD), BF16),
            pltpu.VMEM((segs, 128, HD), BF16),
            pltpu.VMEM((32, width), BF16),
            pltpu.VMEM((32, width), BF16),
            pltpu.VMEM((32, 2 * HD), BF16),
            pltpu.VMEM((2, 9, tok, tok), F32),
            pltpu.VMEM((2, tok, 128), F32),
            pltpu.VMEM((2, tok, 128), F32),
            pltpu.VMEM((2, tok, HD), F32),
            pltpu.VMEM((segs, 8, tok, 2 * HD), BF16),
            pltpu.VMEM((segs, 16, 4, 384), F32),
            pltpu.VMEM((segs, 16, 4, 384), F32),
            pltpu.VMEM((segs, 8, 8, 2 * HD), BF16),
            pltpu.VMEM((segs, 8, 8, 896), BF16),
            pltpu.VMEM((segs, 16, 8, 896), BF16),
            dma((8,)),
            dma((2, segs, 20)),
            dma((2, segs, 16, 2)),
            dma((segs, 8)),
            dma((segs, 8, 2)),
            dma((segs, 16)),
            dma((segs, 16)),
            dma((segs, 8)),
            dma((segs, 8)),
            dma((segs, 8)),
            dma((segs, 8)),
            dma((segs, 16)),
            dma((segs, 16)),
        ],
        compiler_params=pltpu.CompilerParams(
            collective_id=0, has_side_effects=True, vmem_limit_bytes=60000 * 1024),
    )(segment_input, doc_ids, memory, gain, w_query, w_key, w_value, w_out.T, mem_proj)
    return hidden_t.transpose(0, 2, 1), new_memory


def solution(mesh):
    return jax.shard_map(
        per_device,
        mesh=mesh,
        in_specs=(
            P(None, "seq", None),
            P(),
            P(),
            P(),
            P(None, "head"),
            P(None, "head"),
            P(None, "head"),
            P(None, "head"),
            P("head", None),
        ),
        out_specs=(P(None, "seq", "head"), P()),
        check_vma=False,
    )
```

```python
import math

import jax
import jax.numpy as jnp
from jax import lax
from jax.experimental import pallas as pl
from jax.experimental.pallas import tpu as pltpu
from jax.sharding import PartitionSpec as P

HD = 256
MESH = pl.DeviceIdType.MESH
F32 = jnp.float32
BF16 = jnp.bfloat16
NEG = -1e30
EXP_FACTOR = HD ** (-0.5) * math.log2(math.e)


def scoped(f):
    def g(*args):
        with jax.named_scope(f.__name__ + "".join(f"_{a}" for a in args if isinstance(a, int))):
            return f(*args)
    return g


def dot(a, b):
    return jnp.dot(a, b, preferred_element_type=F32)


def dot_t(a, b):
    return lax.dot_general(a, b, (((1,), (1,)), ((), ())), preferred_element_type=F32)


def body(
    x_hbm, docs_hbm, mem_hbm, gain_hbm, wq_hbm, wk_hbm, wv_hbm, wo_hbm, mp_hbm,
    hid_ref, newmem_ref,
    docs_ref, gain_ref, xb, xn, xr, wq, wk, wv, wo, mp, qb, kv, km, vm, nm, memb, qm, sc, mxs, att, ha, ps, po, mg, pr, mb,
    load_sem, kv_send, kv_recv, att_send, att_recv, ps_send, po_recv, mg_send, mg_recv, pr_send, pr_recv, mb_send, mb_recv,
):
    segs, tok, width = x_hbm.shape
    s = lax.axis_index("seq")
    h = lax.axis_index("head")
    y, x = s // 4, s % 4
    z, c = h // 2, h % 2
    cols = wo_hbm.shape[0]

    loads = [
        pltpu.make_async_copy(x_hbm.at[0], xb.at[0], load_sem.at[0]),
        pltpu.make_async_copy(wk_hbm, wk, load_sem.at[1]),
        pltpu.make_async_copy(wv_hbm, wv, load_sem.at[2]),
        pltpu.make_async_copy(x_hbm.at[1], xb.at[1], load_sem.at[3]),
        pltpu.make_async_copy(wq_hbm, wq, load_sem.at[4]),
        pltpu.make_async_copy(mp_hbm, mp, load_sem.at[5]),
        pltpu.make_async_copy(wo_hbm, wo, load_sem.at[6]),
        pltpu.make_async_copy(
            x_hbm.at[:, :, pl.ds(pl.multiple_of(z * 896, 128), 896)], xr, load_sem.at[7]),
    ]
    loads += [
        pltpu.make_async_copy(gain_hbm, gain_ref, load_sem.at[8]),
        pltpu.make_async_copy(mem_hbm, memb, load_sem.at[9]),
        pltpu.make_async_copy(docs_hbm, docs_ref, load_sem.at[10]),
    ]
    for k in (8, 0, 1, 2, 9):
        loads[k].start()

    barrier = pltpu.get_barrier_semaphore()

    @pl.loop(1, 16)
    def _(p):
        pl.semaphore_signal(barrier, inc=1, device_id=((s + p) % 16, h), device_id_type=MESH)

    @pl.loop(1, 8)
    def _(p):
        pl.semaphore_signal(barrier, inc=1, device_id=(s, (h + p) % 8), device_id_type=MESH)

    def remote(src, dst, ssem, rsem, where):
        return pltpu.make_async_remote_copy(
            src_ref=src, dst_ref=dst, send_sem=ssem, recv_sem=rsem, device_id=where, device_id_type=MESH)

    def at(kind, i, j):
        dx, dy = (i, j) if kind == 0 else (j, i)
        return ((y + dy + 4) % 4) * 4 + (x + dx + 4) % 4

    def piece(kind, seg, i, j, half):
        ref = kv.at[kind, seg, at(kind, i, j)]
        return ref if half is None else ref.at[pl.ds(half * 128, 128)]

    def kv_copy(kind, seg, i, j, half, di, dj):
        ref = piece(kind, seg, i, j, half)
        remote(ref, ref, kv_send.at[kind, seg], kv_recv.at[kind, seg, at(kind, i, j), half or 0],
               (at(kind, di, dj), h)).start()

    def kv_wait(kind, seg, i, j):
        halves = (0, 1) if (j == 2 or (i, j) == (2, 0)) else (None,)
        for half in halves:
            ref = piece(kind, seg, i, j, half)
            remote(ref, ref, kv_send.at[kind, seg], kv_recv.at[kind, seg, at(kind, i, j), half or 0],
                   (at(kind, 1, 0), h)).wait_recv()

    @scoped
    def round0(seg):
        for kind in (0, 1):
            for di, dj in ((1, 0), (-1, 0), (0, 1), (0, -1)):
                kv_copy(kind, seg, 0, 0, None, di, dj)

    @scoped
    def round1(seg):
        for kind in (0, 1):
            kv_wait(kind, seg, -1, 0)
            kv_copy(kind, seg, -1, 0, 0, 1, 0)
            kv_copy(kind, seg, -1, 0, None, 0, 1)
            kv_copy(kind, seg, -1, 0, None, 0, -1)
            kv_wait(kind, seg, 1, 0)
            kv_copy(kind, seg, 1, 0, 1, -1, 0)
            kv_copy(kind, seg, 1, 0, None, 0, 1)
            kv_copy(kind, seg, 1, 0, None, 0, -1)
            kv_wait(kind, seg, 0, -1)
            kv_copy(kind, seg, 0, -1, 0, 0, 1)
            kv_wait(kind, seg, 0, 1)
            kv_copy(kind, seg, 0, 1, 1, 0, -1)

    @scoped
    def round2(seg):
        for kind in (0, 1):
            kv_wait(kind, seg, 2, 0)
            kv_copy(kind, seg, 2, 0, None, 0, 1)
            kv_copy(kind, seg, 2, 0, None, 0, -1)
            for i in (-1, 1):
                kv_wait(kind, seg, i, -1)
                kv_copy(kind, seg, i, -1, 0, 0, 1)
                kv_wait(kind, seg, i, 1)
                kv_copy(kind, seg, i, 1, 1, 0, -1)

    @scoped
    def round3(seg):
        for kind in (0, 1):
            kv_wait(kind, seg, 2, -1)
            kv_copy(kind, seg, 2, -1, 0, 0, 1)
            kv_wait(kind, seg, 2, 1)
            kv_copy(kind, seg, 2, 1, 1, 0, -1)

    @scoped
    def round4(seg):
        for kind in (0, 1):
            for i in (0, -1, 1, 2):
                kv_wait(kind, seg, i, 2)

    def head_at(dz, core):
        return ((z + dz + 4) % 4) * 2 + core

    def att_piece(seg, head, g, half):
        ref = att.at[seg, head, g]
        return ref if half is None else ref.at[pl.ds(half * 128, 128)]

    def att_copy(seg, head, g, half, where):
        ref = att_piece(seg, head, g, half)
        remote(ref, ref, att_send.at[seg], att_recv.at[seg, head, g, half or 0], (s, where)).start()

    def att_wait(seg, head, g, half=None):
        ref = att_piece(seg, head, g, half)
        remote(ref, ref, att_send.at[seg], att_recv.at[seg, head, g, half or 0],
               (s, head_at(1, c))).wait_recv()

    other = 1 - c

    @scoped
    def heads0(seg, g):
        att_copy(seg, h, g, None, head_at(1, c))
        att_copy(seg, h, g, None, head_at(-1, c))
        att_copy(seg, h, g, None, head_at(0, other))

    @scoped
    def heads1(seg, g):
        att_wait(seg, head_at(-1, c), g)
        att_copy(seg, head_at(-1, c), g, 0, head_at(1, c))
        att_copy(seg, head_at(-1, c), g, None, head_at(0, other))
        att_wait(seg, head_at(1, c), g)
        att_copy(seg, head_at(1, c), g, 1, head_at(-1, c))
        att_copy(seg, head_at(1, c), g, None, head_at(0, other))

    @scoped
    def heads2(seg, g):
        att_wait(seg, head_at(2, c), g, 0)
        att_wait(seg, head_at(2, c), g, 1)
        att_copy(seg, head_at(2, c), g, None, head_at(0, other))

    @scoped
    def heads3(seg, dz):
        att_wait(seg, head_at(dz, other), 0)
        att_wait(seg, head_at(dz, other), 1)

    def to_owners(seg):
        @pl.loop(1, 16)
        def _(p):
            who = (s + p) % 16
            remote(ps.at[seg, who], po.at[seg, s], ps_send.at[seg], po_recv.at[seg], (who, h)).start()

    @scoped
    def from_owners(seg):
        ref = po.at[seg, pl.ds(0, 15)]
        remote(ref, ref, ps_send.at[seg], po_recv.at[seg], ((s + 1) % 16, h)).wait_recv()

    def to_heads(ref, ssem, rsem, seg):
        @pl.loop(1, 8)
        def _(p):
            remote(ref.at[seg, h], ref.at[seg, h], ssem.at[seg], rsem.at[seg], (s, (h + p) % 8)).start()

    @scoped
    def from_heads(ref, ssem, rsem, seg):
        some = ref.at[seg, pl.ds(0, 7)]
        remote(some, some, ssem.at[seg], rsem.at[seg], (s, (h + 1) % 8)).wait_recv()

    def to_seq(seg):
        @pl.loop(1, 16)
        def _(p):
            remote(mb.at[seg, s], mb.at[seg, s], mb_send.at[seg], mb_recv.at[seg], ((s + p) % 16, h)).start()

    @scoped
    def from_seq(seg):
        ref = mb.at[seg, pl.ds(0, 15)]
        remote(ref, ref, mb_send.at[seg], mb_recv.at[seg], ((s + 1) % 16, h)).wait_recv()

    @scoped
    def all_sent():
        near = ((s + 1) % 16, h)
        for seg in range(2):
            groups = [
                (kv.at[0, seg, pl.ds(0, 15)], kv_send.at[0, seg]),
                (kv.at[1, seg, pl.ds(0, 15)], kv_send.at[1, seg]),
                (att.at[seg, pl.ds(0, 7)], att_send.at[seg]),
                (po.at[seg, pl.ds(0, 15)], ps_send.at[seg]),
                (mg.at[seg, pl.ds(0, 7)], mg_send.at[seg]),
                (pr.at[seg, pl.ds(0, 7)], pr_send.at[seg]),
                (mb.at[seg, pl.ds(0, 15)], mb_send.at[seg]),
            ]
            for ref, sem in groups:
                remote(ref, ref, sem, load_sem.at[0], near).wait_send()


    @scoped
    def norm_tokens(seg):
        gain = gain_ref[...].astype(F32).reshape(1, width)

        @pl.loop(0, tok // 16, unroll=2)
        def _(i):
            rows = pl.ds(pl.multiple_of(i * 16, 16), 16)
            v = xb[seg, rows, :].astype(F32)
            mean = jnp.sum(v * v, axis=-1, keepdims=True) * (1.0 / width)
            xn[seg, rows, :] = (v * lax.rsqrt(mean + 1e-06) * gain).astype(BF16)

    @scoped
    def keys_values(seg):
        kv[0, seg, s] = dot(xn[seg], wk[...]).astype(BF16)
        kv[1, seg, s] = dot(xn[seg], wv[...]).astype(BF16)

    @scoped
    def gather_memory(seg):
        blocks = mb[seg].reshape(128, 896)
        m = lax.broadcasted_iota(jnp.int32, (32, 128), 0)
        j = lax.broadcasted_iota(jnp.int32, (32, 128), 1)
        for yy in range(4):
            pick = (m == (j // 8) * 2 + j % 2) & ((j % 8) // 2 == yy)
            memb[:, 896 * yy:896 * yy + 896] = dot(jnp.where(pick, 1.0, 0.0).astype(BF16), blocks).astype(BF16)

    @scoped
    def project_memory(seg):
        gain = gain_ref[...].astype(F32).reshape(1, width)
        for pair in range(2):
            v = memb[pair * 16:pair * 16 + 16, :].astype(F32)
            mean = jnp.sum(v * v, axis=-1, keepdims=True) * (1.0 / width)
            nm[pair * 16:pair * 16 + 16, :] = (v * lax.rsqrt(mean + 1e-06) * gain).astype(BF16)
        qm[...] = dot(nm[...], wq[...]).astype(BF16)
        km[seg, 0:32, :] = dot(nm[...], wk[...]).astype(BF16)
        vm[seg, 0:32, :] = dot(nm[...], wv[...]).astype(BF16)

    def weights_of(scores, peak):
        return jnp.exp2((scores - peak) * EXP_FACTOR)

    def memory_scores(q, seg):
        lane = lax.broadcasted_iota(jnp.int32, (q.shape[0], 128), 1)
        return jnp.where(lane < 32, dot_t(q, km[seg]), NEG)

    @scoped
    def attend_memory(seg):
        q = jnp.concatenate([qm[:, 0:256], qm[:, 256:512]], axis=0)
        lane = lax.broadcasted_iota(jnp.int32, (64, 128), 1)
        first = jnp.where((lane < 32) & (s == 0), dot_t(q, km[seg]), NEG)
        scores = dot_t(q, kv[0, seg, s])
        peak = jnp.maximum(jnp.max(first, axis=1, keepdims=True), jnp.max(scores, axis=1, keepdims=True))
        w_first = weights_of(first, peak)
        w = weights_of(scores, peak)
        total = jnp.sum(w_first, axis=1, keepdims=True) + jnp.sum(w, axis=1, keepdims=True)
        mixed = dot(w_first.astype(BF16), vm[seg]) + dot(w.astype(BF16), kv[1, seg, s])
        stats = jnp.where(lane < 64, peak, total)
        for t in range(16):
            for g in range(2):
                row = 32 * g + 2 * t
                ps[seg, t, 2 * g:2 * g + 2, 0:256] = mixed[row:row + 2]
                ps[seg, t, 2 * g:2 * g + 2, 256:384] = stats[row:row + 2]
        po[seg, s] = ps[seg, s]

    @scoped
    def combine_memory(seg):
        peaks = [po[seg, t, :, 256:257] for t in range(16)]
        peak = peaks[0]
        for one in peaks[1:]:
            peak = jnp.maximum(peak, one)
        total = jnp.zeros((4, 1), F32)
        mixed = jnp.zeros((4, 256), F32)
        for t in range(16):
            f = weights_of(peaks[t], peak)
            total = total + f * po[seg, t, :, 320:321]
            mixed = mixed + f * po[seg, t, :, 0:256]
        result = mixed / total
        for g in range(2):
            mg[seg, h, :, 256 * g:256 * g + 256] = jnp.concatenate([result[2 * g:2 * g + 2]] * 4, axis=0).astype(BF16)

    @scoped
    def write_memory(seg):
        out = dot_t(mg[seg, 0], wo[:, 0:512])
        for head in range(1, 8):
            out = out + dot_t(mg[seg, head], wo[:, head * 512:head * 512 + 512])
        k = lax.broadcasted_iota(jnp.int32, (8, 32), 0)
        m = lax.broadcasted_iota(jnp.int32, (8, 32), 1)
        own = jnp.where(m == 2 * s + k % 2, 1.0, 0.0).astype(BF16)
        old = dot(own, memb[:, pl.ds(pl.multiple_of(z * 896, 128), 896)])
        old = jnp.where(c == 0, old[:, 0:cols], old[:, cols:2 * cols])
        part = dot((old + out).astype(BF16), mp[...])
        k = lax.broadcasted_iota(jnp.int32, (8, 896), 0)
        block = part[:, 0:896]
        for yy in range(1, 4):
            block = jnp.where(k // 2 == yy, part[:, 896 * yy:896 * yy + 896], block)
        pr[seg, h] = block.astype(BF16)

    @scoped
    def sum_memory(seg):
        total = pr[seg, 0].astype(F32)
        for head in range(1, 8):
            total = total + pr[seg, head].astype(F32)
        mb[seg, s] = total.astype(BF16)

    def first_keys(seg):
        docs = docs_ref[seg:seg + 1, :]
        pos = s * tok + lax.broadcasted_iota(jnp.int32, (tok, 1), 0)
        start = jnp.zeros((tok, 1), jnp.int32)
        for doc in (1, 2, 3):
            begin = jnp.sum(jnp.where(docs < doc, 1, 0), axis=1, keepdims=True)
            start = jnp.maximum(start, jnp.where(begin <= pos, begin, 0))
        return start, pos

    def score_blocks(seg, low, high):
        start, pos = first_keys(seg)

        @pl.loop(low, high)
        def _(d):
            t = s - d
            key_pos = t * tok + lax.broadcasted_iota(jnp.int32, (tok, tok), 1)
            ok = (key_pos >= start) & (key_pos <= pos)
            for g in range(2):
                scores = jnp.where(ok, dot_t(qb[seg, :, g * HD:g * HD + HD], kv[0, seg, t]), NEG)
                sc[g, d] = scores
                mxs[g] = jnp.maximum(mxs[g], jnp.maximum(scores[:, 0:128], scores[:, 128:256]))

    near = jnp.minimum(s, x + 4) + 1
    reach = jnp.minimum(s, 8) + 1

    @scoped
    def scores_near(seg):
        mxs[...] = jnp.full_like(mxs, NEG)
        score_blocks(seg, 0, near)

    @scoped
    def scores_far(seg):
        score_blocks(seg, near, reach)

    @scoped
    def attend(seg, g):
        first = memory_scores(qb[seg, :, g * HD:g * HD + HD], seg)
        peak = jnp.max(jnp.maximum(mxs[g], first), axis=1, keepdims=True)
        w_first = weights_of(first, peak)
        total = w_first
        mixed = dot(w_first.astype(BF16), vm[seg])
        for d in range(9):
            w = weights_of(sc[g, d], peak)
            if d > 0:
                w = jnp.where(d <= s, w, 0.0)
            total = total + (w[:, 0:128] + w[:, 128:256])
            mixed = mixed + dot(w.astype(BF16), kv[1, seg, jnp.maximum(s - d, 0)])
        total = jnp.sum(total, axis=1, keepdims=True)
        att[seg, h, g] = (mixed / total).astype(BF16)

    def head_term(seg, head, out):
        for g in range(2):
            lanes = pl.ds(pl.multiple_of(head * 512 + g * 256, 256), 256)
            out = out + dot_t(wo[:, lanes], att[seg, head, g])
        return out

    @scoped
    def add_heads(seg, *where):
        out = ha[seg]
        for dz, core in where:
            out = head_term(seg, head_at(dz, core), out)
        ha[seg] = out

    @scoped
    def last_heads(seg, *where):
        out = ha[seg]
        for dz, core in where:
            out = head_term(seg, head_at(dz, core), out)
        hid_ref[seg] = out.astype(BF16)

    @scoped
    def residual(seg):
        old = xr[seg].astype(F32).T
        ha[seg] = jnp.where(c == 0, old[0:cols], old[cols:2 * cols])

    km[...] = jnp.zeros_like(km)
    vm[...] = jnp.zeros_like(vm)
    with jax.named_scope("load0"):
        loads[8].wait()
        loads[0].wait()
    for k in (4, 3):
        loads[k].start()
    norm_tokens(0)
    with jax.named_scope("load1"):
        loads[1].wait()
        loads[2].wait()
    for k in (6, 5, 7, 10):
        loads[k].start()
    keys_values(0)
    with jax.named_scope("barrier"):
        pl.semaphore_wait(barrier, 22)
    round0(0)
    with jax.named_scope("load4"):
        loads[4].wait()
        loads[9].wait()
    project_memory(0)
    attend_memory(0)
    to_owners(0)
    with jax.named_scope("load3"):
        loads[3].wait()
    norm_tokens(1)
    keys_values(1)
    round1(0)
    round0(1)
    with jax.named_scope("query"):
        qb[0] = dot(xn[0], wq[...]).astype(BF16)
    from_owners(0)
    combine_memory(0)
    to_heads(mg, mg_send, mg_recv, 0)
    with jax.named_scope("query"):
        qb[1] = dot(xn[1], wq[...]).astype(BF16)
    for k in (5, 6, 7, 10):
        loads[k].wait()
    from_heads(mg, mg_send, mg_recv, 0)
    write_memory(0)
    to_heads(pr, pr_send, pr_recv, 0)
    round2(0)
    residual(0)
    residual(1)
    from_heads(pr, pr_send, pr_recv, 0)
    sum_memory(0)
    to_seq(0)
    round1(1)
    round3(0)
    scores_near(0)
    from_seq(0)
    gather_memory(0)
    project_memory(1)
    attend_memory(1)
    to_owners(1)
    round2(1)
    round4(0)
    scores_far(0)
    attend(0, 0)
    heads0(0, 0)
    attend(0, 1)
    heads0(0, 1)
    round3(1)
    from_owners(1)
    combine_memory(1)
    to_heads(mg, mg_send, mg_recv, 1)
    scores_near(1)
    heads1(0, 0)
    from_heads(mg, mg_send, mg_recv, 1)
    write_memory(1)
    to_heads(pr, pr_send, pr_recv, 1)
    heads1(0, 1)
    round4(1)
    scores_far(1)
    attend(1, 0)
    heads0(1, 0)
    attend(1, 1)
    heads0(1, 1)
    from_heads(pr, pr_send, pr_recv, 1)
    sum_memory(1)
    to_seq(1)
    heads2(0, 0)
    heads2(0, 1)
    add_heads(0, (0, c), (-1, c), (1, c), (2, c))
    heads1(1, 0)
    for dz in (0, -1, 1, 2):
        heads3(0, dz)
    last_heads(0, (0, other), (-1, other), (1, other), (2, other))
    heads1(1, 1)
    from_seq(1)
    gather_memory(1)
    newmem_ref[...] = memb[...]
    add_heads(1, (0, c), (-1, c), (1, c))
    heads2(1, 0)
    for dz in (0, -1, 1):
        heads3(1, dz)
    add_heads(1, (0, other), (-1, other), (1, other))
    heads2(1, 1)
    add_heads(1, (2, c))
    heads3(1, 2)
    last_heads(1, (2, other))

    all_sent()


def per_device(segment_input, doc_ids, memory, gain, w_query, w_key, w_value, w_out, mem_proj):
    segs, tok, width = segment_input.shape
    cols = w_out.shape[1]
    anywhere = pl.BlockSpec(memory_space=pl.ANY)
    vmem = pl.BlockSpec(memory_space=pltpu.VMEM)
    dma = pltpu.SemaphoreType.DMA
    hidden_t, new_memory = pl.pallas_call(
        body,
        out_shape=(
            jax.ShapeDtypeStruct((segs, cols, tok), BF16),
            jax.ShapeDtypeStruct(memory.shape, BF16),
        ),
        in_specs=[anywhere] * 9,
        out_specs=(vmem, vmem),
        scratch_shapes=[
            pltpu.VMEM(doc_ids.shape, jnp.int32),
            pltpu.VMEM(gain.shape, BF16),
            pltpu.VMEM((segs, tok, width), BF16),
            pltpu.VMEM((segs, tok, width), BF16),
            pltpu.VMEM((segs, tok, 896), BF16),
            pltpu.VMEM(w_query.shape, BF16),
            pltpu.VMEM(w_key.shape, BF16),
            pltpu.VMEM(w_value.shape, BF16),
            pltpu.VMEM((cols, w_out.shape[0]), BF16),
            pltpu.VMEM(mem_proj.shape, BF16),
            pltpu.VMEM((segs, tok, 2 * HD), BF16),
            pltpu.VMEM((2, segs, 16, tok, HD), BF16),
            pltpu.VMEM((segs, 128, HD), BF16),
            pltpu.VMEM((segs, 128, HD), BF16),
            pltpu.VMEM((32, width), BF16),
            pltpu.VMEM((32, width), BF16),
            pltpu.VMEM((32, 2 * HD), BF16),
            pltpu.VMEM((2, 9, tok, tok), F32),
            pltpu.VMEM((2, tok, 128), F32),
            pltpu.VMEM((segs, 8, 2, tok, HD), BF16),
            pltpu.VMEM((segs, cols, tok), F32),
            pltpu.VMEM((segs, 16, 4, 384), F32),
            pltpu.VMEM((segs, 16, 4, 384), F32),
            pltpu.VMEM((segs, 8, 8, 2 * HD), BF16),
            pltpu.VMEM((segs, 8, 8, 896), BF16),
            pltpu.VMEM((segs, 16, 8, 896), BF16),
            dma((11,)),
            dma((2, segs)),
            dma((2, segs, 16, 2)),
            dma((segs,)),
            dma((segs, 8, 2, 2)),
            dma((segs,)),
            dma((segs,)),
            dma((segs,)),
            dma((segs,)),
            dma((segs,)),
            dma((segs,)),
            dma((segs,)),
            dma((segs,)),
        ],
        compiler_params=pltpu.CompilerParams(
            collective_id=0, has_side_effects=True, vmem_limit_bytes=60000 * 1024),
    )(segment_input, doc_ids, memory, gain, w_query, w_key, w_value, w_out.T, mem_proj)
    return hidden_t.transpose(0, 2, 1), new_memory


def solution(mesh):
    return jax.shard_map(
        per_device,
        mesh=mesh,
        in_specs=(
            P(None, "seq", None),
            P(),
            P(),
            P(),
            P(None, "head"),
            P(None, "head"),
            P(None, "head"),
            P(None, "head"),
            P("head", None),
        ),
        out_specs=(P(None, "seq", "head"), P()),
        check_vma=False,
    )
```

```python
import math

import jax
import jax.numpy as jnp
from jax import lax
from jax.experimental import pallas as pl
from jax.experimental.pallas import tpu as pltpu
from jax.sharding import PartitionSpec as P

HD = 256
MESH = pl.DeviceIdType.MESH
F32 = jnp.float32
BF16 = jnp.bfloat16
NEG = -1e30
EXP_FACTOR = HD ** (-0.5) * math.log2(math.e)


def scoped(f):
    def g(*args):
        with jax.named_scope(f.__name__ + "".join(f"_{a}" for a in args if isinstance(a, int))):
            return f(*args)
    return g


def dot(a, b):
    return jnp.dot(a, b, preferred_element_type=F32)


def dot_t(a, b):
    return lax.dot_general(a, b, (((1,), (1,)), ((), ())), preferred_element_type=F32)


def body(
    x_hbm, docs_hbm, mem_hbm, gain_hbm, wq_hbm, wk_hbm, wv_hbm, wo_hbm, mp_hbm,
    hid_ref, newmem_ref,
    docs_ref, gain_ref, xb, xn, xr, wq, wk, wv, wo, mp, qb, kv, km, vm, nm, memb, qm, sc, mxs, att, ha, ps, po, mg, pr, mb,
    load_sem, kv_send, kv_recv, att_send, att_recv, ps_send, po_recv, mg_send, mg_recv, pr_send, pr_recv, mb_send, mb_recv,
):
    segs, tok, width = x_hbm.shape
    s = lax.axis_index("seq")
    h = lax.axis_index("head")
    y, x = s // 4, s % 4
    z, c = h // 2, h % 2
    cols = wo_hbm.shape[0]

    loads = [
        pltpu.make_async_copy(x_hbm.at[0], xb.at[0], load_sem.at[0]),
        pltpu.make_async_copy(wk_hbm, wk, load_sem.at[1]),
        pltpu.make_async_copy(wv_hbm, wv, load_sem.at[2]),
        pltpu.make_async_copy(x_hbm.at[1], xb.at[1], load_sem.at[3]),
        pltpu.make_async_copy(wq_hbm, wq, load_sem.at[4]),
        pltpu.make_async_copy(mp_hbm, mp, load_sem.at[5]),
        pltpu.make_async_copy(wo_hbm, wo, load_sem.at[6]),
        pltpu.make_async_copy(
            x_hbm.at[:, :, pl.ds(pl.multiple_of(z * 896, 128), 896)], xr, load_sem.at[7]),
    ]
    loads += [
        pltpu.make_async_copy(gain_hbm, gain_ref, load_sem.at[8]),
        pltpu.make_async_copy(mem_hbm, memb, load_sem.at[9]),
        pltpu.make_async_copy(docs_hbm, docs_ref, load_sem.at[10]),
    ]
    for k in (8, 0, 1, 2, 9):
        loads[k].start()

    barrier = pltpu.get_barrier_semaphore()

    @pl.loop(1, 16)
    def _(p):
        pl.semaphore_signal(barrier, inc=1, device_id=((s + p) % 16, h), device_id_type=MESH)

    @pl.loop(1, 8)
    def _(p):
        pl.semaphore_signal(barrier, inc=1, device_id=(s, (h + p) % 8), device_id_type=MESH)

    def remote(src, dst, ssem, rsem, where):
        return pltpu.make_async_remote_copy(
            src_ref=src, dst_ref=dst, send_sem=ssem, recv_sem=rsem, device_id=where, device_id_type=MESH)

    def at(kind, i, j):
        dx, dy = (i, j) if kind == 0 else (j, i)
        return ((y + dy + 4) % 4) * 4 + (x + dx + 4) % 4

    not_last = y <= 2
    early = y <= 1
    middle = (y >= 1) & (y <= 2)
    relay = (y == 0) | (y == 3)
    has_one = y >= 1
    has_two = y >= 2
    sent = {}

    def on(cond, f):
        if cond is None:
            f()
        else:
            pl.when(cond)(f)

    def cut_rows(kind, along):
        return 96 if (kind == 0) == (along == 2) else 128

    def piece(kind, seg, i, j, half, along):
        ref = kv.at[kind, seg, at(kind, i, j)]
        at_row = cut_rows(kind, along)
        if half is None:
            return ref, 256
        if half == 0:
            return ref.at[pl.ds(0, at_row)], at_row
        return ref.at[pl.ds(at_row, 256 - at_row)], 256 - at_row

    def kv_copy(kind, seg, i, j, half, di, dj, name=None, cond=None):
        ref, rows = piece(kind, seg, i, j, half, 1 if di else 2)
        group = sent.setdefault((kind, seg), {})
        group[name] = (cond, group.get(name, (cond, 0))[1] + rows)
        on(cond, lambda: remote(
            ref, ref, kv_send.at[kind, seg], kv_recv.at[kind, seg, at(kind, i, j), half or 0],
            (at(kind, di, dj), h)).start())

    def kv_wait(kind, seg, i, j, cond=None, halves=None):
        along = 2
        if halves is None:
            halves = (None,)
            if j == 2:
                halves = (0, 1)
            elif (i, j) == (2, 0):
                halves, along = (0, 1), 1
        elif j == 0:
            along = 1

        def wait():
            for half in halves:
                ref, _ = piece(kind, seg, i, j, half, along)
                remote(ref, ref, kv_send.at[kind, seg], kv_recv.at[kind, seg, at(kind, i, j), half or 0],
                       (at(kind, 1, 0), h)).wait_recv()

        on(cond, wait)

    def up_down(seg, i):
        kv_copy(0, seg, i, 0, None, 0, 1, "not_last", not_last)
        kv_copy(0, seg, i, 0, 1, 0, -1, "early", early)

    def relay_keys(seg, i):
        kv_wait(0, seg, i, -1, has_one)
        kv_copy(0, seg, i, -1, 0, 0, 1, "middle", middle)
        kv_wait(0, seg, i, 1, relay, (1,))
        kv_copy(0, seg, i, 1, 1, 0, -1, "relay", relay)

    def relay_values(seg, i, name, cond):
        kv_wait(1, seg, i, -1, cond)
        kv_copy(1, seg, i, -1, 0, 0, 1, name, cond)
        kv_wait(1, seg, i, 1, cond)
        kv_copy(1, seg, i, 1, 1, 0, -1, name, cond)

    def both_sides(kind, seg, i, name, cond):
        di, dj = (1, 0) if kind == 0 else (0, 1)
        kv_copy(kind, seg, i, 0, None, di, dj, name, cond)
        kv_copy(kind, seg, i, 0, None, -di, -dj, name, cond)

    @scoped
    def round0(seg, *kinds):
        if 0 in kinds:
            both_sides(0, seg, 0, None, None)
            up_down(seg, 0)
        if 1 in kinds:
            kv_copy(1, seg, 0, 0, None, 1, 0, "not_last", not_last)
            kv_copy(1, seg, 0, 0, 1, -1, 0, "early", early)
            both_sides(1, seg, 0, None, None)

    @scoped
    def round1(seg):
        kv_wait(0, seg, -1, 0)
        kv_copy(0, seg, -1, 0, 0, 1, 0)
        up_down(seg, -1)
        kv_wait(0, seg, 1, 0)
        kv_copy(0, seg, 1, 0, 1, -1, 0)
        up_down(seg, 1)
        relay_keys(seg, 0)
        kv_wait(1, seg, -1, 0, has_one)
        kv_copy(1, seg, -1, 0, 0, 1, 0, "middle", middle)
        both_sides(1, seg, -1, "has_one", has_one)
        kv_wait(1, seg, 1, 0, relay, (1,))
        kv_copy(1, seg, 1, 0, 1, -1, 0, "relay", relay)
        relay_values(seg, 0, None, None)

    @scoped
    def round2(seg):
        kv_wait(0, seg, 2, 0)
        up_down(seg, 2)
        kv_wait(1, seg, 2, 0, has_two)
        both_sides(1, seg, 2, "has_two", has_two)
        relay_keys(seg, -1)
        relay_keys(seg, 1)
        relay_values(seg, -1, "has_one", has_one)

    @scoped
    def round3(seg):
        relay_keys(seg, 2)
        relay_values(seg, 2, "has_two", has_two)

    @scoped
    def round4(seg):
        for i in (0, -1, 1, 2):
            kv_wait(0, seg, i, 2, has_two)
        kv_wait(1, seg, 0, 2)
        kv_wait(1, seg, -1, 2, has_one)
        kv_wait(1, seg, 2, 2, has_two)

    def head_at(dz, core):
        return ((z + dz + 4) % 4) * 2 + core

    def att_piece(seg, head, g, half):
        ref = att.at[seg, head, g]
        return ref if half is None else ref.at[pl.ds(half * 128, 128)]

    def att_copy(seg, head, g, half, where):
        ref = att_piece(seg, head, g, half)
        remote(ref, ref, att_send.at[seg], att_recv.at[seg, head, g, half or 0], (s, where)).start()

    def att_wait(seg, head, g, half=None):
        ref = att_piece(seg, head, g, half)
        remote(ref, ref, att_send.at[seg], att_recv.at[seg, head, g, half or 0],
               (s, head_at(1, c))).wait_recv()

    other = 1 - c

    @scoped
    def heads0(seg, g):
        att_copy(seg, h, g, None, head_at(1, c))
        att_copy(seg, h, g, None, head_at(-1, c))
        att_copy(seg, h, g, None, head_at(0, other))

    @scoped
    def heads1(seg, g):
        att_wait(seg, head_at(-1, c), g)
        att_copy(seg, head_at(-1, c), g, 0, head_at(1, c))
        att_copy(seg, head_at(-1, c), g, None, head_at(0, other))
        att_wait(seg, head_at(1, c), g)
        att_copy(seg, head_at(1, c), g, 1, head_at(-1, c))
        att_copy(seg, head_at(1, c), g, None, head_at(0, other))

    @scoped
    def heads2(seg, g):
        att_wait(seg, head_at(2, c), g, 0)
        att_wait(seg, head_at(2, c), g, 1)
        att_copy(seg, head_at(2, c), g, None, head_at(0, other))

    @scoped
    def heads3(seg, dz):
        att_wait(seg, head_at(dz, other), 0)
        att_wait(seg, head_at(dz, other), 1)

    def to_owners(seg):
        @pl.loop(1, 16)
        def _(p):
            who = (s + p) % 16
            remote(ps.at[seg, who], po.at[seg, s], ps_send.at[seg], po_recv.at[seg], (who, h)).start()

    @scoped
    def from_owners(seg):
        ref = po.at[seg, pl.ds(0, 15)]
        remote(ref, ref, ps_send.at[seg], po_recv.at[seg], ((s + 1) % 16, h)).wait_recv()

    def to_heads(ref, ssem, rsem, seg):
        @pl.loop(1, 8)
        def _(p):
            remote(ref.at[seg, h], ref.at[seg, h], ssem.at[seg], rsem.at[seg], (s, (h + p) % 8)).start()

    @scoped
    def from_heads(ref, ssem, rsem, seg):
        some = ref.at[seg, pl.ds(0, 7)]
        remote(some, some, ssem.at[seg], rsem.at[seg], (s, (h + 1) % 8)).wait_recv()

    def to_seq(seg):
        @pl.loop(1, 16)
        def _(p):
            remote(mb.at[seg, s], mb.at[seg, s], mb_send.at[seg], mb_recv.at[seg], ((s + p) % 16, h)).start()

    @scoped
    def from_seq(seg):
        ref = mb.at[seg, pl.ds(0, 15)]
        remote(ref, ref, mb_send.at[seg], mb_recv.at[seg], ((s + 1) % 16, h)).wait_recv()

    @scoped
    def all_sent():
        near = ((s + 1) % 16, h)
        for seg in range(2):
            groups = [
                (att.at[seg, pl.ds(0, 7)], att_send.at[seg]),
                (po.at[seg, pl.ds(0, 15)], ps_send.at[seg]),
                (mg.at[seg, pl.ds(0, 7)], mg_send.at[seg]),
                (pr.at[seg, pl.ds(0, 7)], pr_send.at[seg]),
                (mb.at[seg, pl.ds(0, 15)], mb_send.at[seg]),
            ]
            for ref, sem in groups:
                remote(ref, ref, sem, load_sem.at[0], near).wait_send()
        for (kind, seg), group in sent.items():
            for cond, rows in group.values():
                whole, rest = rows // 256, rows % 256
                refs = [kv.at[kind, seg, pl.ds(0, whole)]] if whole else []
                if rest:
                    refs.append(kv.at[kind, seg, 0, pl.ds(0, rest)])

                def wait(refs=refs, sem=kv_send.at[kind, seg]):
                    for ref in refs:
                        remote(ref, ref, sem, load_sem.at[0], near).wait_send()

                on(cond, wait)


    @scoped
    def norm_tokens(seg):
        gain = gain_ref[...].astype(F32).reshape(1, width)

        @pl.loop(0, tok // 16, unroll=2)
        def _(i):
            rows = pl.ds(pl.multiple_of(i * 16, 16), 16)
            v = xb[seg, rows, :].astype(F32)
            mean = jnp.sum(v * v, axis=-1, keepdims=True) * (1.0 / width)
            xn[seg, rows, :] = (v * lax.rsqrt(mean + 1e-06) * gain).astype(BF16)

    @scoped
    def keys_values(seg):
        kv[0, seg, s] = dot(xn[seg], wk[...]).astype(BF16)
        kv[1, seg, s] = dot(xn[seg], wv[...]).astype(BF16)

    @scoped
    def gather_memory(seg):
        blocks = mb[seg].reshape(128, 896)
        m = lax.broadcasted_iota(jnp.int32, (32, 128), 0)
        j = lax.broadcasted_iota(jnp.int32, (32, 128), 1)
        for yy in range(4):
            pick = (m == (j // 8) * 2 + j % 2) & ((j % 8) // 2 == yy)
            memb[:, 896 * yy:896 * yy + 896] = dot(jnp.where(pick, 1.0, 0.0).astype(BF16), blocks).astype(BF16)

    @scoped
    def project_memory(seg):
        gain = gain_ref[...].astype(F32).reshape(1, width)
        for pair in range(2):
            v = memb[pair * 16:pair * 16 + 16, :].astype(F32)
            mean = jnp.sum(v * v, axis=-1, keepdims=True) * (1.0 / width)
            nm[pair * 16:pair * 16 + 16, :] = (v * lax.rsqrt(mean + 1e-06) * gain).astype(BF16)
        qm[...] = dot(nm[...], wq[...]).astype(BF16)
        km[seg, 0:32, :] = dot(nm[...], wk[...]).astype(BF16)
        vm[seg, 0:32, :] = dot(nm[...], wv[...]).astype(BF16)

    def weights_of(scores, peak):
        return jnp.exp2((scores - peak) * EXP_FACTOR)

    def memory_scores(q, seg):
        lane = lax.broadcasted_iota(jnp.int32, (q.shape[0], 128), 1)
        return jnp.where(lane < 32, dot_t(q, km[seg]), NEG)

    @scoped
    def attend_memory(seg):
        q = jnp.concatenate([qm[:, 0:256], qm[:, 256:512]], axis=0)
        lane = lax.broadcasted_iota(jnp.int32, (64, 128), 1)
        first = jnp.where((lane < 32) & (s == 0), dot_t(q, km[seg]), NEG)
        scores = dot_t(q, kv[0, seg, s])
        peak = jnp.maximum(jnp.max(first, axis=1, keepdims=True), jnp.max(scores, axis=1, keepdims=True))
        w_first = weights_of(first, peak)
        w = weights_of(scores, peak)
        total = jnp.sum(w_first, axis=1, keepdims=True) + jnp.sum(w, axis=1, keepdims=True)
        mixed = dot(w_first.astype(BF16), vm[seg]) + dot(w.astype(BF16), kv[1, seg, s])
        stats = jnp.where(lane < 64, peak, total)
        for t in range(16):
            for g in range(2):
                row = 32 * g + 2 * t
                ps[seg, t, 2 * g:2 * g + 2, 0:256] = mixed[row:row + 2]
                ps[seg, t, 2 * g:2 * g + 2, 256:384] = stats[row:row + 2]
        po[seg, s] = ps[seg, s]

    @scoped
    def combine_memory(seg):
        peaks = [po[seg, t, :, 256:257] for t in range(16)]
        peak = peaks[0]
        for one in peaks[1:]:
            peak = jnp.maximum(peak, one)
        total = jnp.zeros((4, 1), F32)
        mixed = jnp.zeros((4, 256), F32)
        for t in range(16):
            f = weights_of(peaks[t], peak)
            total = total + f * po[seg, t, :, 320:321]
            mixed = mixed + f * po[seg, t, :, 0:256]
        result = mixed / total
        for g in range(2):
            mg[seg, h, :, 256 * g:256 * g + 256] = jnp.concatenate([result[2 * g:2 * g + 2]] * 4, axis=0).astype(BF16)

    @scoped
    def write_memory(seg):
        out = dot_t(mg[seg, 0], wo[:, 0:512])
        for head in range(1, 8):
            out = out + dot_t(mg[seg, head], wo[:, head * 512:head * 512 + 512])
        k = lax.broadcasted_iota(jnp.int32, (8, 32), 0)
        m = lax.broadcasted_iota(jnp.int32, (8, 32), 1)
        own = jnp.where(m == 2 * s + k % 2, 1.0, 0.0).astype(BF16)
        old = dot(own, memb[:, pl.ds(pl.multiple_of(z * 896, 128), 896)])
        old = jnp.where(c == 0, old[:, 0:cols], old[:, cols:2 * cols])
        part = dot((old + out).astype(BF16), mp[...])
        k = lax.broadcasted_iota(jnp.int32, (8, 896), 0)
        block = part[:, 0:896]
        for yy in range(1, 4):
            block = jnp.where(k // 2 == yy, part[:, 896 * yy:896 * yy + 896], block)
        pr[seg, h] = block.astype(BF16)

    @scoped
    def sum_memory(seg):
        total = pr[seg, 0].astype(F32)
        for head in range(1, 8):
            total = total + pr[seg, head].astype(F32)
        mb[seg, s] = total.astype(BF16)

    def first_keys(seg):
        docs = docs_ref[seg:seg + 1, :]
        pos = s * tok + lax.broadcasted_iota(jnp.int32, (tok, 1), 0)
        start = jnp.zeros((tok, 1), jnp.int32)
        for doc in (1, 2, 3):
            begin = jnp.sum(jnp.where(docs < doc, 1, 0), axis=1, keepdims=True)
            start = jnp.maximum(start, jnp.where(begin <= pos, begin, 0))
        return start, pos

    def score_blocks(seg, low, high):
        start, pos = first_keys(seg)

        @pl.loop(low, high)
        def _(d):
            t = s - d
            key_pos = t * tok + lax.broadcasted_iota(jnp.int32, (tok, tok), 1)
            ok = (key_pos >= start) & (key_pos <= pos)
            for g in range(2):
                scores = jnp.where(ok, dot_t(qb[seg, :, g * HD:g * HD + HD], kv[0, seg, t]), NEG)
                sc[g, d] = scores
                mxs[g] = jnp.maximum(mxs[g], jnp.maximum(scores[:, 0:128], scores[:, 128:256]))

    near = jnp.minimum(s, x + 4) + 1
    reach = jnp.minimum(s, 8) + 1

    @scoped
    def scores_near(seg):
        mxs[...] = jnp.full_like(mxs, NEG)
        score_blocks(seg, 0, near)

    @scoped
    def scores_far(seg):
        score_blocks(seg, near, reach)

    @scoped
    def attend(seg, g):
        first = memory_scores(qb[seg, :, g * HD:g * HD + HD], seg)
        peak = jnp.max(jnp.maximum(mxs[g], first), axis=1, keepdims=True)
        w_first = weights_of(first, peak)
        total = w_first
        mixed = dot(w_first.astype(BF16), vm[seg])
        for d in range(9):
            w = weights_of(sc[g, d], peak)
            if d > 0:
                w = jnp.where(d <= s, w, 0.0)
            total = total + (w[:, 0:128] + w[:, 128:256])
            mixed = mixed + dot(w.astype(BF16), kv[1, seg, jnp.maximum(s - d, 0)])
        total = jnp.sum(total, axis=1, keepdims=True)
        att[seg, h, g] = (mixed / total).astype(BF16)

    def head_term(seg, head, out):
        for g in range(2):
            lanes = pl.ds(pl.multiple_of(head * 512 + g * 256, 256), 256)
            out = out + dot_t(wo[:, lanes], att[seg, head, g])
        return out

    @scoped
    def add_heads(seg, *where):
        out = ha[seg]
        for dz, core in where:
            out = head_term(seg, head_at(dz, core), out)
        ha[seg] = out

    @scoped
    def last_heads(seg, *where):
        out = ha[seg]
        for dz, core in where:
            out = head_term(seg, head_at(dz, core), out)
        hid_ref[seg] = out.astype(BF16)

    @scoped
    def residual(seg):
        old = xr[seg].astype(F32).T
        ha[seg] = jnp.where(c == 0, old[0:cols], old[cols:2 * cols])

    km[...] = jnp.zeros_like(km)
    vm[...] = jnp.zeros_like(vm)
    with jax.named_scope("load0"):
        loads[8].wait()
        loads[0].wait()
    for k in (4, 3):
        loads[k].start()
    norm_tokens(0)
    with jax.named_scope("load1"):
        loads[1].wait()
        loads[2].wait()
    for k in (6, 5, 7, 10):
        loads[k].start()
    keys_values(0)
    with jax.named_scope("barrier"):
        pl.semaphore_wait(barrier, 22)
    round0(0, 0)
    with jax.named_scope("load4"):
        loads[4].wait()
        loads[9].wait()
    project_memory(0)
    attend_memory(0)
    to_owners(0)
    round0(0, 1)
    with jax.named_scope("load3"):
        loads[3].wait()
    norm_tokens(1)
    keys_values(1)
    from_owners(0)
    combine_memory(0)
    to_heads(mg, mg_send, mg_recv, 0)
    round1(0)
    with jax.named_scope("query"):
        qb[0] = dot(xn[0], wq[...]).astype(BF16)
    for k in (5, 6, 7, 10):
        loads[k].wait()
    from_heads(mg, mg_send, mg_recv, 0)
    write_memory(0)
    to_heads(pr, pr_send, pr_recv, 0)
    round2(0)
    from_heads(pr, pr_send, pr_recv, 0)
    sum_memory(0)
    to_seq(0)
    round0(1, 0, 1)
    with jax.named_scope("query"):
        qb[1] = dot(xn[1], wq[...]).astype(BF16)
    residual(0)
    residual(1)
    round3(0)
    scores_near(0)
    from_seq(0)
    gather_memory(0)
    project_memory(1)
    attend_memory(1)
    to_owners(1)
    round1(1)
    from_owners(1)
    combine_memory(1)
    to_heads(mg, mg_send, mg_recv, 1)
    round4(0)
    scores_far(0)
    attend(0, 0)
    heads0(0, 0)
    attend(0, 1)
    heads0(0, 1)
    round2(1)
    from_heads(mg, mg_send, mg_recv, 1)
    write_memory(1)
    to_heads(pr, pr_send, pr_recv, 1)
    heads1(0, 0)
    round3(1)
    heads1(0, 1)
    scores_near(1)
    round4(1)
    scores_far(1)
    attend(1, 0)
    heads0(1, 0)
    attend(1, 1)
    heads0(1, 1)
    from_heads(pr, pr_send, pr_recv, 1)
    sum_memory(1)
    to_seq(1)
    heads2(0, 0)
    heads2(0, 1)
    add_heads(0, (0, c), (-1, c), (1, c), (2, c))
    for dz in (0, -1, 1, 2):
        heads3(0, dz)
    last_heads(0, (0, other), (-1, other), (1, other), (2, other))
    heads1(1, 0)
    add_heads(1, (0, c))
    heads1(1, 1)
    add_heads(1, (-1, c), (1, c))
    heads2(1, 0)
    from_seq(1)
    gather_memory(1)
    newmem_ref[...] = memb[...]
    for dz in (0, -1, 1):
        heads3(1, dz)
    add_heads(1, (0, other), (-1, other), (1, other))
    heads2(1, 1)
    add_heads(1, (2, c))
    heads3(1, 2)
    last_heads(1, (2, other))
    all_sent()


def per_device(segment_input, doc_ids, memory, gain, w_query, w_key, w_value, w_out, mem_proj):
    segs, tok, width = segment_input.shape
    cols = w_out.shape[1]
    anywhere = pl.BlockSpec(memory_space=pl.ANY)
    vmem = pl.BlockSpec(memory_space=pltpu.VMEM)
    dma = pltpu.SemaphoreType.DMA
    hidden_t, new_memory = pl.pallas_call(
        body,
        out_shape=(
            pltpu.VMEM((segs, cols, tok), BF16),
            pltpu.VMEM(memory.shape, BF16),
        ),
        in_specs=[anywhere] * 9,
        out_specs=(vmem, vmem),
        scratch_shapes=[
            pltpu.VMEM(doc_ids.shape, jnp.int32),
            pltpu.VMEM(gain.shape, BF16),
            pltpu.VMEM((segs, tok, width), BF16),
            pltpu.VMEM((segs, tok, width), BF16),
            pltpu.VMEM((segs, tok, 896), BF16),
            pltpu.VMEM(w_query.shape, BF16),
            pltpu.VMEM(w_key.shape, BF16),
            pltpu.VMEM(w_value.shape, BF16),
            pltpu.VMEM((cols, w_out.shape[0]), BF16),
            pltpu.VMEM(mem_proj.shape, BF16),
            pltpu.VMEM((segs, tok, 2 * HD), BF16),
            pltpu.VMEM((2, segs, 16, tok, HD), BF16),
            pltpu.VMEM((segs, 128, HD), BF16),
            pltpu.VMEM((segs, 128, HD), BF16),
            pltpu.VMEM((32, width), BF16),
            pltpu.VMEM((32, width), BF16),
            pltpu.VMEM((32, 2 * HD), BF16),
            pltpu.VMEM((2, 9, tok, tok), F32),
            pltpu.VMEM((2, tok, 128), F32),
            pltpu.VMEM((segs, 8, 2, tok, HD), BF16),
            pltpu.VMEM((segs, cols, tok), F32),
            pltpu.VMEM((segs, 16, 4, 384), F32),
            pltpu.VMEM((segs, 16, 4, 384), F32),
            pltpu.VMEM((segs, 8, 8, 2 * HD), BF16),
            pltpu.VMEM((segs, 8, 8, 896), BF16),
            pltpu.VMEM((segs, 16, 8, 896), BF16),
            dma((11,)),
            dma((2, segs)),
            dma((2, segs, 16, 2)),
            dma((segs,)),
            dma((segs, 8, 2, 2)),
            dma((segs,)),
            dma((segs,)),
            dma((segs,)),
            dma((segs,)),
            dma((segs,)),
            dma((segs,)),
            dma((segs,)),
            dma((segs,)),
        ],
        compiler_params=pltpu.CompilerParams(
            collective_id=0, has_side_effects=True, vmem_limit_bytes=60000 * 1024),
    )(segment_input, doc_ids, memory, gain, w_query, w_key, w_value, w_out.T, mem_proj)
    return hidden_t.transpose(0, 2, 1), new_memory


def solution(mesh):
    return jax.shard_map(
        per_device,
        mesh=mesh,
        in_specs=(
            P(None, "seq", None),
            P(),
            P(),
            P(),
            P(None, "head"),
            P(None, "head"),
            P(None, "head"),
            P(None, "head"),
            P("head", None),
        ),
        out_specs=(P(None, "seq", "head"), P()),
        check_vma=False,
    )
```

```python
import math

import jax
import jax.numpy as jnp
from jax import lax
from jax.experimental import pallas as pl
from jax.experimental.pallas import tpu as pltpu
from jax.sharding import PartitionSpec as P

HD = 256
MESH = pl.DeviceIdType.MESH
F32 = jnp.float32
BF16 = jnp.bfloat16
NEG = -1e30
EXP_FACTOR = HD ** (-0.5) * math.log2(math.e)


def scoped(f):
    def g(*args):
        with jax.named_scope(f.__name__ + "".join(f"_{a}" for a in args if isinstance(a, int))):
            return f(*args)
    return g


def dot(a, b):
    return jnp.dot(a, b, preferred_element_type=F32)


def dot_t(a, b):
    return lax.dot_general(a, b, (((1,), (1,)), ((), ())), preferred_element_type=F32)


def body(
    x_hbm, docs_hbm, mem_hbm, gain_hbm, wq_hbm, wk_hbm, wv_hbm, wo_hbm, mp_hbm,
    hid_ref, newmem_ref,
    docs_ref, gain_ref, xb, xn, xr, wq, wk, wv, wo, mp, qb, kv, km, vm, nm, memb, qm, sc, mxs, att, ha, ps, po, mg, pr, mb,
    load_sem, kv_send, kv_recv, att_send, att_recv, ps_send, po_recv, mg_send, mg_recv, pr_send, pr_recv, mb_send, mb_recv,
):
    segs, tok, width = x_hbm.shape
    s = lax.axis_index("seq")
    h = lax.axis_index("head")
    y, x = s // 4, s % 4
    z, c = h // 2, h % 2
    cols = wo_hbm.shape[0]

    loads = [
        pltpu.make_async_copy(x_hbm.at[0], xb.at[0], load_sem.at[0]),
        pltpu.make_async_copy(wk_hbm, wk, load_sem.at[1]),
        pltpu.make_async_copy(wv_hbm, wv, load_sem.at[2]),
        pltpu.make_async_copy(x_hbm.at[1], xb.at[1], load_sem.at[3]),
        pltpu.make_async_copy(wq_hbm, wq, load_sem.at[4]),
        pltpu.make_async_copy(mp_hbm, mp, load_sem.at[5]),
        pltpu.make_async_copy(wo_hbm, wo, load_sem.at[6]),
        pltpu.make_async_copy(
            x_hbm.at[:, :, pl.ds(pl.multiple_of(z * 896, 128), 896)], xr, load_sem.at[7]),
    ]
    loads += [
        pltpu.make_async_copy(gain_hbm, gain_ref, load_sem.at[8]),
        pltpu.make_async_copy(mem_hbm, memb, load_sem.at[9]),
        pltpu.make_async_copy(docs_hbm, docs_ref, load_sem.at[10]),
    ]
    for k in (8, 0, 1, 2, 9):
        loads[k].start()

    barrier = pltpu.get_barrier_semaphore()

    @pl.loop(1, 16)
    def _(p):
        pl.semaphore_signal(barrier, inc=1, device_id=((s + p) % 16, h), device_id_type=MESH)

    @pl.loop(1, 8)
    def _(p):
        pl.semaphore_signal(barrier, inc=1, device_id=(s, (h + p) % 8), device_id_type=MESH)

    def remote(src, dst, ssem, rsem, where):
        return pltpu.make_async_remote_copy(
            src_ref=src, dst_ref=dst, send_sem=ssem, recv_sem=rsem, device_id=where, device_id_type=MESH)

    def at(kind, i, j):
        dx, dy = (i, j) if kind == 0 else (j, i)
        return ((y + dy + 4) % 4) * 4 + (x + dx + 4) % 4

    not_last = y <= 2
    early = y <= 1
    middle = (y >= 1) & (y <= 2)
    relay = (y == 0) | (y == 3)
    has_one = y >= 1
    has_two = y >= 2
    sent = {}

    def on(cond, f):
        if cond is None:
            f()
        else:
            pl.when(cond)(f)

    def cut_rows(kind, along):
        return 96 if (kind == 0) == (along == 2) else 128

    def piece(kind, seg, i, j, half, along):
        ref = kv.at[kind, seg, at(kind, i, j)]
        at_row = cut_rows(kind, along)
        if half is None:
            return ref, 256
        if half == 0:
            return ref.at[pl.ds(0, at_row)], at_row
        return ref.at[pl.ds(at_row, 256 - at_row)], 256 - at_row

    slots = (
        {(-1, 0): 0, (1, 0): 1, (2, 0): 2, (0, -1): 3, (-1, -1): 4, (1, -1): 5, (2, -1): 6, (0, 1): 7,
         (-1, 1): 8, (1, 1): 9, (2, 1): 10, (0, 2): 11, (-1, 2): 11, (1, 2): 11, (2, 2): 11},
        {(-1, 0): 0, (1, 0): 1, (2, 0): 2, (0, -1): 3, (0, 1): 4, (-1, -1): 5, (-1, 1): 6, (2, -1): 7,
         (2, 1): 8, (0, 2): 9, (-1, 2): 10, (2, 2): 11},
    )

    def seen(kind, i, j):
        return slots[kind][((i + 5) % 4 - 1, (j + 5) % 4 - 1)]

    def kv_copy(kind, seg, i, j, half, di, dj, name=None, cond=None):
        ref, rows = piece(kind, seg, i, j, half, 1 if di else 2)
        group = sent.setdefault((kind, seg), {})
        group[name] = (cond, group.get(name, (cond, 0))[1] + rows)
        on(cond, lambda: remote(
            ref, ref, kv_send.at[kind, seg], kv_recv.at[kind, seg, seen(kind, i - di, j - dj)],
            (at(kind, di, dj), h)).start())

    def kv_wait(kind, seg, i, j, cond=None, half=None):
        ref, _ = piece(kind, seg, i, j, half, 1 if j == 0 else 2)

        def wait(ref=ref):
            remote(ref, ref, kv_send.at[kind, seg], kv_recv.at[kind, seg, seen(kind, i, j)],
                   (at(kind, 1, 0), h)).wait_recv()

        on(cond, wait)

    def up_down(seg, i):
        kv_copy(0, seg, i, 0, None, 0, 1, "not_last", not_last)
        kv_copy(0, seg, i, 0, 1, 0, -1, "early", early)

    def relay_keys(seg, i):
        kv_wait(0, seg, i, -1, has_one)
        kv_copy(0, seg, i, -1, 0, 0, 1, "middle", middle)
        kv_wait(0, seg, i, 1, relay, 1)
        kv_copy(0, seg, i, 1, 1, 0, -1, "relay", relay)

    def relay_values(seg, i, name, cond):
        kv_wait(1, seg, i, -1, cond)
        kv_copy(1, seg, i, -1, 0, 0, 1, name, cond)
        kv_wait(1, seg, i, 1, cond)
        kv_copy(1, seg, i, 1, 1, 0, -1, name, cond)

    def both_sides(kind, seg, i, name, cond):
        di, dj = (1, 0) if kind == 0 else (0, 1)
        kv_copy(kind, seg, i, 0, None, di, dj, name, cond)
        kv_copy(kind, seg, i, 0, None, -di, -dj, name, cond)

    @scoped
    def round0(seg, *kinds):
        if 0 in kinds:
            both_sides(0, seg, 0, None, None)
            up_down(seg, 0)
        if 1 in kinds:
            kv_copy(1, seg, 0, 0, None, 1, 0, "not_last", not_last)
            kv_copy(1, seg, 0, 0, 1, -1, 0, "early", early)
            both_sides(1, seg, 0, None, None)

    @scoped
    def round1_keys(seg):
        kv_wait(0, seg, -1, 0)
        kv_copy(0, seg, -1, 0, 0, 1, 0)
        up_down(seg, -1)
        kv_wait(0, seg, 1, 0)
        kv_copy(0, seg, 1, 0, 1, -1, 0)
        up_down(seg, 1)
        relay_keys(seg, 0)

    @scoped
    def round1_values(seg):
        kv_wait(1, seg, -1, 0, has_one)
        kv_copy(1, seg, -1, 0, 0, 1, 0, "middle", middle)
        both_sides(1, seg, -1, "has_one", has_one)
        kv_wait(1, seg, 1, 0, relay, 1)
        kv_copy(1, seg, 1, 0, 1, -1, 0, "relay", relay)
        relay_values(seg, 0, None, None)

    @scoped
    def round2(seg):
        kv_wait(0, seg, 2, 0)
        up_down(seg, 2)
        kv_wait(1, seg, 2, 0, has_two)
        both_sides(1, seg, 2, "has_two", has_two)
        relay_keys(seg, -1)
        relay_keys(seg, 1)
        relay_values(seg, -1, "has_one", has_one)

    @scoped
    def round3(seg):
        relay_keys(seg, 2)
        relay_values(seg, 2, "has_two", has_two)

    @scoped
    def round4(seg):
        @pl.when(has_two)
        def _():
            ref = kv.at[0, seg, pl.ds(0, 4)]
            remote(ref, ref, kv_send.at[0, seg], kv_recv.at[0, seg, 11], (at(0, 1, 0), h)).wait_recv()

        kv_wait(1, seg, 0, 2)
        kv_wait(1, seg, -1, 2, has_one)
        kv_wait(1, seg, 2, 2, has_two)

    def head_at(dz, core):
        return ((z + dz + 4) % 4) * 2 + core

    other = 1 - c

    def att_piece(seg, head, g, half):
        ref = att.at[seg, head, g]
        return ref if half is None else ref.at[pl.ds(half * 128, 128)]

    def att_copy(seg, dz, g, half, to, slot):
        head, where = head_at(dz, c), head_at(to, c if slot < 6 else other)
        ref = att_piece(seg, head, g, half)
        remote(ref, ref, att_send.at[seg], att_recv.at[seg, slot], (s, where)).start()

    def att_wait(seg, ref, slot):
        remote(ref, ref, att_send.at[seg], att_recv.at[seg, slot], (s, head_at(1, c))).wait_recv()

    @scoped
    def heads0(seg, g):
        att_copy(seg, 0, g, None, 1, g)
        att_copy(seg, 0, g, None, -1, 2 + g)
        att_copy(seg, 0, g, None, 0, 6)

    @scoped
    def heads1(seg, g):
        att_wait(seg, att.at[seg, head_at(-1, c), g], g)
        att_copy(seg, -1, g, 0, 1, 4 + g)
        att_copy(seg, -1, g, None, 0, 7)
        att_wait(seg, att.at[seg, head_at(1, c), g], 2 + g)
        att_copy(seg, 1, g, 1, -1, 4 + g)
        att_copy(seg, 1, g, None, 0, 8)

    @scoped
    def heads2(seg, g):
        att_wait(seg, att.at[seg, head_at(2, c), g], 4 + g)
        att_copy(seg, 2, g, None, 0, 9)

    @scoped
    def heads3(seg, dz):
        att_wait(seg, att.at[seg, head_at(dz, other)], 6 + (0, -1, 1, 2).index(dz))

    def to_owners(seg):
        @pl.loop(1, 16)
        def _(p):
            who = (s + p) % 16
            remote(ps.at[seg, who], po.at[seg, s], ps_send.at[seg], po_recv.at[seg], (who, h)).start()

    @scoped
    def from_owners(seg):
        ref = po.at[seg, pl.ds(0, 15)]
        remote(ref, ref, ps_send.at[seg], po_recv.at[seg], ((s + 1) % 16, h)).wait_recv()

    def to_heads(ref, ssem, rsem, seg):
        @pl.loop(1, 8)
        def _(p):
            remote(ref.at[seg, h], ref.at[seg, h], ssem.at[seg], rsem.at[seg], (s, (h + p) % 8)).start()

    @scoped
    def from_heads(ref, ssem, rsem, seg):
        some = ref.at[seg, pl.ds(0, 7)]
        remote(some, some, ssem.at[seg], rsem.at[seg], (s, (h + 1) % 8)).wait_recv()

    def to_seq(seg):
        @pl.loop(1, 16)
        def _(p):
            remote(mb.at[seg, s], mb.at[seg, s], mb_send.at[seg], mb_recv.at[seg], ((s + p) % 16, h)).start()

    @scoped
    def from_seq(seg):
        ref = mb.at[seg, pl.ds(0, 15)]
        remote(ref, ref, mb_send.at[seg], mb_recv.at[seg], ((s + 1) % 16, h)).wait_recv()

    @scoped
    def all_sent():
        near = ((s + 1) % 16, h)
        for seg in range(2):
            groups = [
                (att.at[seg, pl.ds(0, 7)], att_send.at[seg]),
                (po.at[seg, pl.ds(0, 15)], ps_send.at[seg]),
                (mg.at[seg, pl.ds(0, 7)], mg_send.at[seg]),
                (pr.at[seg, pl.ds(0, 7)], pr_send.at[seg]),
            ]
            groups.append((mb.at[seg, pl.ds(0, 15)], mb_send.at[seg]))
            for ref, sem in groups:
                remote(ref, ref, sem, load_sem.at[0], near).wait_send()
        for (kind, seg), group in sent.items():
            for cond, rows in group.values():
                whole, rest = rows // 256, rows % 256
                refs = [kv.at[kind, seg, pl.ds(0, whole)]] if whole else []
                if rest:
                    refs.append(kv.at[kind, seg, 0, pl.ds(0, rest)])

                def wait(refs=refs, sem=kv_send.at[kind, seg]):
                    for ref in refs:
                        remote(ref, ref, sem, load_sem.at[0], near).wait_send()

                on(cond, wait)


    @scoped
    def norm_tokens(seg):
        gain = gain_ref[...].astype(F32).reshape(1, width)

        @pl.loop(0, tok // 16, unroll=2)
        def _(i):
            rows = pl.ds(pl.multiple_of(i * 16, 16), 16)
            v = xb[seg, rows, :].astype(F32)
            mean = jnp.sum(v * v, axis=-1, keepdims=True) * (1.0 / width)
            xn[seg, rows, :] = (v * lax.rsqrt(mean + 1e-06) * gain).astype(BF16)

    @scoped
    def keys_values(seg):
        kv[0, seg, s] = dot(xn[seg], wk[...]).astype(BF16)
        kv[1, seg, s] = dot(xn[seg], wv[...]).astype(BF16)

    @scoped
    def gather_memory(seg):
        m = lax.broadcasted_iota(jnp.int32, (32, 128), 0)
        j = lax.broadcasted_iota(jnp.int32, (32, 128), 1)
        blocks = mb[seg].reshape(128, 896)
        for yy in range(4):
            pick = (m == (j // 8) * 2 + j % 2) & ((j % 8) // 2 == yy)
            memb[:, 896 * yy:896 * yy + 896] = dot(jnp.where(pick, 1.0, 0.0).astype(BF16), blocks).astype(BF16)

    @scoped
    def project_memory(seg):
        gain = gain_ref[...].astype(F32).reshape(1, width)
        for pair in range(2):
            v = memb[pair * 16:pair * 16 + 16, :].astype(F32)
            mean = jnp.sum(v * v, axis=-1, keepdims=True) * (1.0 / width)
            nm[pair * 16:pair * 16 + 16, :] = (v * lax.rsqrt(mean + 1e-06) * gain).astype(BF16)
        qm[...] = dot(nm[...], wq[...]).astype(BF16)
        km[seg, 0:32, :] = dot(nm[...], wk[...]).astype(BF16)
        vm[seg, 0:32, :] = dot(nm[...], wv[...]).astype(BF16)

    def weights_of(scores, peak):
        return jnp.exp2((scores - peak) * EXP_FACTOR)

    def memory_scores(q, seg):
        lane = lax.broadcasted_iota(jnp.int32, (q.shape[0], 128), 1)
        return jnp.where(lane < 32, dot_t(q, km[seg]), NEG)

    @scoped
    def attend_memory(seg):
        q = jnp.concatenate([qm[:, 0:256], qm[:, 256:512]], axis=0)
        lane = lax.broadcasted_iota(jnp.int32, (64, 128), 1)
        first = jnp.where((lane < 32) & (s == 0), dot_t(q, km[seg]), NEG)
        scores = dot_t(q, kv[0, seg, s])
        peak = jnp.maximum(jnp.max(first, axis=1, keepdims=True), jnp.max(scores, axis=1, keepdims=True))
        w_first = weights_of(first, peak)
        w = weights_of(scores, peak)
        total = jnp.sum(w_first, axis=1, keepdims=True) + jnp.sum(w, axis=1, keepdims=True)
        mixed = dot(w_first.astype(BF16), vm[seg]) + dot(w.astype(BF16), kv[1, seg, s])
        stats = jnp.where(lane < 64, peak, total)
        for t in range(16):
            for g in range(2):
                row = 32 * g + 2 * t
                ps[seg, t, 2 * g:2 * g + 2, 0:256] = mixed[row:row + 2]
                ps[seg, t, 2 * g:2 * g + 2, 256:384] = stats[row:row + 2]
        po[seg, s] = ps[seg, s]

    @scoped
    def combine_memory(seg):
        peaks = [po[seg, t, :, 256:257] for t in range(16)]
        peak = peaks[0]
        for one in peaks[1:]:
            peak = jnp.maximum(peak, one)
        total = jnp.zeros((4, 1), F32)
        mixed = jnp.zeros((4, 256), F32)
        for t in range(16):
            f = weights_of(peaks[t], peak)
            total = total + f * po[seg, t, :, 320:321]
            mixed = mixed + f * po[seg, t, :, 0:256]
        result = mixed / total
        for g in range(2):
            mg[seg, h, :, 256 * g:256 * g + 256] = jnp.concatenate([result[2 * g:2 * g + 2]] * 4, axis=0).astype(BF16)

    @scoped
    def write_memory(seg):
        out = dot_t(mg[seg, 0], wo[:, 0:512])
        for head in range(1, 8):
            out = out + dot_t(mg[seg, head], wo[:, head * 512:head * 512 + 512])
        k = lax.broadcasted_iota(jnp.int32, (8, 32), 0)
        m = lax.broadcasted_iota(jnp.int32, (8, 32), 1)
        own = jnp.where(m == 2 * s + k % 2, 1.0, 0.0).astype(BF16)
        old = dot(own, memb[:, pl.ds(pl.multiple_of(z * 896, 128), 896)])
        old = jnp.where(c == 0, old[:, 0:cols], old[:, cols:2 * cols])
        part = dot((old + out).astype(BF16), mp[...])
        k = lax.broadcasted_iota(jnp.int32, (8, 896), 0)
        block = part[:, 0:896]
        for yy in range(1, 4):
            block = jnp.where(k // 2 == yy, part[:, 896 * yy:896 * yy + 896], block)
        pr[seg, h] = block.astype(BF16)

    @scoped
    def sum_memory(seg):
        total = pr[seg, 0].astype(F32)
        for head in range(1, 8):
            total = total + pr[seg, head].astype(F32)
        mb[seg, s] = total.astype(BF16)

    def first_keys(seg):
        docs = docs_ref[seg:seg + 1, :]
        pos = s * tok + lax.broadcasted_iota(jnp.int32, (tok, 1), 0)
        start = jnp.zeros((tok, 1), jnp.int32)
        for doc in (1, 2, 3):
            begin = jnp.sum(jnp.where(docs < doc, 1, 0), axis=1, keepdims=True)
            start = jnp.maximum(start, jnp.where(begin <= pos, begin, 0))
        return start, pos

    def score_blocks(seg, low, high):
        start, pos = first_keys(seg)

        @pl.loop(low, high)
        def _(d):
            t = s - d
            key_pos = t * tok + lax.broadcasted_iota(jnp.int32, (tok, tok), 1)
            ok = (key_pos >= start) & (key_pos <= pos)
            for g in range(2):
                scores = jnp.where(ok, dot_t(qb[seg, :, g * HD:g * HD + HD], kv[0, seg, t]), NEG)
                sc[g, d] = scores
                mxs[g] = jnp.maximum(mxs[g], jnp.maximum(scores[:, 0:128], scores[:, 128:256]))

    near = jnp.minimum(s, x + 4) + 1
    reach = jnp.minimum(s, 8) + 1

    @scoped
    def scores_near(seg):
        mxs[...] = jnp.full_like(mxs, NEG)
        score_blocks(seg, 0, near)

    @scoped
    def scores_far(seg):
        score_blocks(seg, near, reach)

    @scoped
    def attend(seg, g):
        first = memory_scores(qb[seg, :, g * HD:g * HD + HD], seg)
        peak = jnp.max(jnp.maximum(mxs[g], first), axis=1, keepdims=True)
        w_first = weights_of(first, peak)
        total = w_first
        mixed = dot(w_first.astype(BF16), vm[seg])
        for d in range(9):
            w = weights_of(sc[g, d], peak)
            if d > 0:
                w = jnp.where(d <= s, w, 0.0)
            total = total + (w[:, 0:128] + w[:, 128:256])
            mixed = mixed + dot(w.astype(BF16), kv[1, seg, jnp.maximum(s - d, 0)])
        total = jnp.sum(total, axis=1, keepdims=True)
        att[seg, h, g] = (mixed / total).astype(BF16)

    def head_term(seg, head, out):
        for g in range(2):
            lanes = pl.ds(pl.multiple_of(head * 512 + g * 256, 256), 256)
            out = out + dot_t(wo[:, lanes], att[seg, head, g])
        return out

    @scoped
    def add_heads(seg, *where):
        out = ha[seg]
        for dz, core in where:
            out = head_term(seg, head_at(dz, core), out)
        ha[seg] = out

    @scoped
    def last_heads(seg, *where):
        out = ha[seg]
        for dz, core in where:
            out = head_term(seg, head_at(dz, core), out)
        hid_ref[seg] = out.astype(BF16)

    @scoped
    def residual(seg):
        old = xr[seg].astype(F32).T
        ha[seg] = jnp.where(c == 0, old[0:cols], old[cols:2 * cols])

    km[...] = jnp.zeros_like(km)
    vm[...] = jnp.zeros_like(vm)
    with jax.named_scope("load0"):
        loads[8].wait()
        loads[0].wait()
    for k in (4, 3):
        loads[k].start()
    norm_tokens(0)
    with jax.named_scope("load1"):
        loads[1].wait()
        loads[2].wait()
    for k in (6, 5, 7, 10):
        loads[k].start()
    keys_values(0)
    with jax.named_scope("barrier"):
        pl.semaphore_wait(barrier, 22)
    round0(0, 0)
    with jax.named_scope("load4"):
        loads[4].wait()
        loads[9].wait()
    project_memory(0)
    attend_memory(0)
    to_owners(0)
    round0(0, 1)
    with jax.named_scope("load3"):
        loads[3].wait()
    norm_tokens(1)
    keys_values(1)
    from_owners(0)
    combine_memory(0)
    to_heads(mg, mg_send, mg_recv, 0)
    round1_keys(0)
    round1_values(0)
    with jax.named_scope("query"):
        qb[0] = dot(xn[0], wq[...]).astype(BF16)
    for k in (5, 6, 7, 10):
        loads[k].wait()
    from_heads(mg, mg_send, mg_recv, 0)
    write_memory(0)
    to_heads(pr, pr_send, pr_recv, 0)
    round2(0)
    from_heads(pr, pr_send, pr_recv, 0)
    sum_memory(0)
    to_seq(0)
    round0(1, 0, 1)
    with jax.named_scope("query"):
        qb[1] = dot(xn[1], wq[...]).astype(BF16)
    residual(0)
    residual(1)
    round3(0)
    scores_near(0)
    from_seq(0)
    gather_memory(0)
    project_memory(1)
    attend_memory(1)
    to_owners(1)
    round1_keys(1)
    round1_values(1)
    round4(0)
    scores_far(0)
    attend(0, 0)
    heads0(0, 0)
    attend(0, 1)
    heads0(0, 1)
    from_owners(1)
    combine_memory(1)
    to_heads(mg, mg_send, mg_recv, 1)
    round2(1)
    heads1(0, 0)
    round3(1)
    heads1(0, 1)
    scores_near(1)
    from_heads(mg, mg_send, mg_recv, 1)
    write_memory(1)
    to_heads(pr, pr_send, pr_recv, 1)
    round4(1)
    scores_far(1)
    attend(1, 0)
    heads0(1, 0)
    heads2(0, 0)
    heads2(0, 1)
    attend(1, 1)
    heads0(1, 1)
    add_heads(0, (0, c), (-1, c), (1, c), (2, c))
    heads1(1, 0)
    for dz in (0, -1, 1, 2):
        heads3(0, dz)
    last_heads(0, (0, other), (-1, other), (1, other), (2, other))
    from_heads(pr, pr_send, pr_recv, 1)
    sum_memory(1)
    to_seq(1)
    heads1(1, 1)
    add_heads(1, (0, c), (-1, c), (1, c))
    heads2(1, 0)
    for dz in (0, -1, 1):
        heads3(1, dz)
    add_heads(1, (0, other), (-1, other), (1, other))
    heads2(1, 1)
    from_seq(1)
    gather_memory(1)
    newmem_ref[...] = memb[...]
    add_heads(1, (2, c))
    heads3(1, 2)
    last_heads(1, (2, other))
    all_sent()


def per_device(segment_input, doc_ids, memory, gain, w_query, w_key, w_value, w_out, mem_proj):
    segs, tok, width = segment_input.shape
    cols = w_out.shape[1]
    anywhere = pl.BlockSpec(memory_space=pl.ANY)
    vmem = pl.BlockSpec(memory_space=pltpu.VMEM)
    dma = pltpu.SemaphoreType.DMA
    hidden_t, new_memory = pl.pallas_call(
        body,
        out_shape=(
            pltpu.VMEM((segs, cols, tok), BF16),
            pltpu.VMEM(memory.shape, BF16),
        ),
        in_specs=[anywhere] * 9,
        out_specs=(vmem, vmem),
        scratch_shapes=[
            pltpu.VMEM(doc_ids.shape, jnp.int32),
            pltpu.VMEM(gain.shape, BF16),
            pltpu.VMEM((segs, tok, width), BF16),
            pltpu.VMEM((segs, tok, width), BF16),
            pltpu.VMEM((segs, tok, 896), BF16),
            pltpu.VMEM(w_query.shape, BF16),
            pltpu.VMEM(w_key.shape, BF16),
            pltpu.VMEM(w_value.shape, BF16),
            pltpu.VMEM((cols, w_out.shape[0]), BF16),
            pltpu.VMEM(mem_proj.shape, BF16),
            pltpu.VMEM((segs, tok, 2 * HD), BF16),
            pltpu.VMEM((2, segs, 16, tok, HD), BF16),
            pltpu.VMEM((segs, 128, HD), BF16),
            pltpu.VMEM((segs, 128, HD), BF16),
            pltpu.VMEM((32, width), BF16),
            pltpu.VMEM((32, width), BF16),
            pltpu.VMEM((32, 2 * HD), BF16),
            pltpu.VMEM((2, 9, tok, tok), F32),
            pltpu.VMEM((2, tok, 128), F32),
            pltpu.VMEM((segs, 8, 2, tok, HD), BF16),
            pltpu.VMEM((segs, cols, tok), F32),
            pltpu.VMEM((segs, 16, 4, 384), F32),
            pltpu.VMEM((segs, 16, 4, 384), F32),
            pltpu.VMEM((segs, 8, 8, 2 * HD), BF16),
            pltpu.VMEM((segs, 8, 8, 896), BF16),
            pltpu.VMEM((segs, 16, 8, 896), BF16),
            dma((11,)),
            dma((2, segs)),
            dma((2, segs, 12)),
            dma((segs,)),
            dma((segs, 10)),
            dma((segs,)),
            dma((segs,)),
            dma((segs,)),
            dma((segs,)),
            dma((segs,)),
            dma((segs,)),
            dma((segs,)),
            dma((segs,)),
        ],
        compiler_params=pltpu.CompilerParams(
            collective_id=0, has_side_effects=True, vmem_limit_bytes=60000 * 1024),
    )(segment_input, doc_ids, memory, gain, w_query, w_key, w_value, w_out.T, mem_proj)
    return hidden_t.transpose(0, 2, 1), new_memory


def solution(mesh):
    return jax.shard_map(
        per_device,
        mesh=mesh,
        in_specs=(
            P(None, "seq", None),
            P(),
            P(),
            P(),
            P(None, "head"),
            P(None, "head"),
            P(None, "head"),
            P(None, "head"),
            P("head", None),
        ),
        out_specs=(P(None, "seq", "head"), P()),
        check_vma=False,
    )
```

```python
import math

import jax
import jax.numpy as jnp
from jax import lax
from jax.experimental import pallas as pl
from jax.experimental.pallas import tpu as pltpu
from jax.sharding import PartitionSpec as P

HD = 256
MESH = pl.DeviceIdType.MESH
F32 = jnp.float32
BF16 = jnp.bfloat16
NEG = -1e30
EXP_FACTOR = HD ** (-0.5) * math.log2(math.e)


def scoped(f):
    def g(*args):
        with jax.named_scope(f.__name__ + "".join(f"_{a}" for a in args if isinstance(a, int))):
            return f(*args)
    return g


def dot(a, b):
    return jnp.dot(a, b, preferred_element_type=F32)


def dot_t(a, b):
    return lax.dot_general(a, b, (((1,), (1,)), ((), ())), preferred_element_type=F32)


def body(
    x_hbm, docs_hbm, mem_hbm, gain_hbm, wq_hbm, wk_hbm, wv_hbm, wo_hbm, mp_hbm,
    hid_ref, newmem_ref,
    docs_ref, gain_ref, xb, xn, xr, wq, wk, wv, wo, mp, qb, kv, km, vm, nm, memb, qm, sc, mxs, att, ha, ps, po, mg, pr, mb,
    load_sem, kv_send, kv_recv, att_send, att_recv, ps_send, po_recv, mg_send, mg_recv, pr_send, pr_recv, mb_send, mb_recv,
):
    segs, tok, width = x_hbm.shape
    s = lax.axis_index("seq")
    h = lax.axis_index("head")
    y, x = s // 4, s % 4
    z, c = h // 2, h % 2
    cols = wo_hbm.shape[0]

    loads = [
        pltpu.make_async_copy(x_hbm.at[0], xb.at[0], load_sem.at[0]),
        pltpu.make_async_copy(wk_hbm, wk, load_sem.at[1]),
        pltpu.make_async_copy(wv_hbm, wv, load_sem.at[2]),
        pltpu.make_async_copy(x_hbm.at[1], xb.at[1], load_sem.at[3]),
        pltpu.make_async_copy(wq_hbm, wq, load_sem.at[4]),
        pltpu.make_async_copy(mp_hbm, mp, load_sem.at[5]),
        pltpu.make_async_copy(wo_hbm, wo, load_sem.at[6]),
        pltpu.make_async_copy(
            x_hbm.at[:, :, pl.ds(pl.multiple_of(z * 896, 128), 896)], xr, load_sem.at[7]),
    ]
    loads += [
        pltpu.make_async_copy(gain_hbm, gain_ref, load_sem.at[8]),
        pltpu.make_async_copy(mem_hbm, memb, load_sem.at[9]),
        pltpu.make_async_copy(docs_hbm, docs_ref, load_sem.at[10]),
    ]
    for k in (8, 0, 1, 2, 9):
        loads[k].start()

    barrier = pltpu.get_barrier_semaphore()

    @pl.loop(1, 16)
    def _(p):
        pl.semaphore_signal(barrier, inc=1, device_id=((s + p) % 16, h), device_id_type=MESH)

    @pl.loop(1, 8)
    def _(p):
        pl.semaphore_signal(barrier, inc=1, device_id=(s, (h + p) % 8), device_id_type=MESH)

    def remote(src, dst, ssem, rsem, where):
        return pltpu.make_async_remote_copy(
            src_ref=src, dst_ref=dst, send_sem=ssem, recv_sem=rsem, device_id=where, device_id_type=MESH)

    def at(kind, i, j):
        dx, dy = (i, j) if kind == 0 else (j, i)
        return ((y + dy + 4) % 4) * 4 + (x + dx + 4) % 4

    not_last = y <= 2
    early = y <= 1
    middle = (y >= 1) & (y <= 2)
    relay = (y == 0) | (y == 3)
    has_one = y >= 1
    has_two = y >= 2
    sent = {}

    def on(cond, f):
        if cond is None:
            f()
        else:
            pl.when(cond)(f)

    def cut_rows(kind, along):
        return 96 if (kind == 0) == (along == 2) else 128

    def piece(kind, seg, i, j, half, along):
        ref = kv.at[kind, seg, at(kind, i, j)]
        at_row = cut_rows(kind, along)
        if half is None:
            return ref, 256
        if half == 0:
            return ref.at[pl.ds(0, at_row)], at_row
        return ref.at[pl.ds(at_row, 256 - at_row)], 256 - at_row

    slots = (
        {(-1, 0): 0, (1, 0): 1, (2, 0): 2, (0, -1): 3, (-1, -1): 4, (1, -1): 5, (2, -1): 6, (0, 1): 7,
         (-1, 1): 8, (1, 1): 9, (2, 1): 10, (0, 2): 11, (-1, 2): 11, (1, 2): 11, (2, 2): 11},
        {(-1, 0): 0, (1, 0): 1, (2, 0): 2, (0, -1): 3, (0, 1): 4, (-1, -1): 5, (-1, 1): 6, (2, -1): 7,
         (2, 1): 8, (0, 2): 9, (-1, 2): 10, (2, 2): 11},
    )

    def seen(kind, i, j):
        return slots[kind][((i + 5) % 4 - 1, (j + 5) % 4 - 1)]

    def kv_copy(kind, seg, i, j, half, di, dj, name=None, cond=None):
        ref, rows = piece(kind, seg, i, j, half, 1 if di else 2)
        group = sent.setdefault((kind, seg), {})
        group[name] = (cond, group.get(name, (cond, 0))[1] + rows)
        on(cond, lambda: remote(
            ref, ref, kv_send.at[kind, seg], kv_recv.at[kind, seg, seen(kind, i - di, j - dj)],
            (at(kind, di, dj), h)).start())

    def kv_wait(kind, seg, i, j, cond=None, half=None):
        ref, _ = piece(kind, seg, i, j, half, 1 if j == 0 else 2)

        def wait(ref=ref):
            remote(ref, ref, kv_send.at[kind, seg], kv_recv.at[kind, seg, seen(kind, i, j)],
                   (at(kind, 1, 0), h)).wait_recv()

        on(cond, wait)

    def up_down(seg, i):
        kv_copy(0, seg, i, 0, None, 0, 1, "not_last", not_last)
        kv_copy(0, seg, i, 0, 1, 0, -1, "early", early)

    def relay_keys(seg, i):
        kv_wait(0, seg, i, -1, has_one)
        kv_copy(0, seg, i, -1, 0, 0, 1, "middle", middle)
        kv_wait(0, seg, i, 1, relay, 1)
        kv_copy(0, seg, i, 1, 1, 0, -1, "relay", relay)

    def relay_values(seg, i, name, cond):
        kv_wait(1, seg, i, -1, cond)
        kv_copy(1, seg, i, -1, 0, 0, 1, name, cond)
        kv_wait(1, seg, i, 1, cond)
        kv_copy(1, seg, i, 1, 1, 0, -1, name, cond)

    def both_sides(kind, seg, i, name, cond):
        di, dj = (1, 0) if kind == 0 else (0, 1)
        kv_copy(kind, seg, i, 0, None, di, dj, name, cond)
        kv_copy(kind, seg, i, 0, None, -di, -dj, name, cond)

    @scoped
    def round0(seg, *kinds):
        if 0 in kinds:
            both_sides(0, seg, 0, None, None)
            up_down(seg, 0)
        if 1 in kinds:
            kv_copy(1, seg, 0, 0, None, 1, 0, "not_last", not_last)
            kv_copy(1, seg, 0, 0, 1, -1, 0, "early", early)
            both_sides(1, seg, 0, None, None)

    @scoped
    def round1_keys(seg):
        kv_wait(0, seg, -1, 0)
        kv_copy(0, seg, -1, 0, 0, 1, 0)
        up_down(seg, -1)
        kv_wait(0, seg, 1, 0)
        kv_copy(0, seg, 1, 0, 1, -1, 0)
        up_down(seg, 1)
        relay_keys(seg, 0)

    @scoped
    def round1_values(seg):
        kv_wait(1, seg, -1, 0, has_one)
        kv_copy(1, seg, -1, 0, 0, 1, 0, "middle", middle)
        both_sides(1, seg, -1, "has_one", has_one)
        kv_wait(1, seg, 1, 0, relay, 1)
        kv_copy(1, seg, 1, 0, 1, -1, 0, "relay", relay)
        relay_values(seg, 0, None, None)

    @scoped
    def round2(seg):
        kv_wait(0, seg, 2, 0)
        up_down(seg, 2)
        kv_wait(1, seg, 2, 0, has_two)
        both_sides(1, seg, 2, "has_two", has_two)
        relay_keys(seg, -1)
        relay_keys(seg, 1)
        relay_values(seg, -1, "has_one", has_one)

    @scoped
    def round3(seg):
        relay_keys(seg, 2)
        relay_values(seg, 2, "has_two", has_two)

    @scoped
    def round4(seg):
        @pl.when(has_two)
        def _():
            ref = kv.at[0, seg, pl.ds(0, 4)]
            remote(ref, ref, kv_send.at[0, seg], kv_recv.at[0, seg, 11], (at(0, 1, 0), h)).wait_recv()

        kv_wait(1, seg, 0, 2)
        kv_wait(1, seg, -1, 2, has_one)
        kv_wait(1, seg, 2, 2, has_two)

    def head_at(dz, core):
        return ((z + dz + 4) % 4) * 2 + core

    other = 1 - c

    def att_piece(seg, head, g, half):
        ref = att.at[seg, head, g]
        return ref if half is None else ref.at[pl.ds(half * 128, 128)]

    def att_copy(seg, dz, g, half, to, slot):
        head, where = head_at(dz, c), head_at(to, c if slot < 6 else other)
        ref = att_piece(seg, head, g, half)
        remote(ref, ref, att_send.at[seg], att_recv.at[seg, slot], (s, where)).start()

    def att_wait(seg, ref, slot):
        remote(ref, ref, att_send.at[seg], att_recv.at[seg, slot], (s, head_at(1, c))).wait_recv()

    @scoped
    def heads0(seg, g):
        att_copy(seg, 0, g, None, 1, g)
        att_copy(seg, 0, g, None, -1, 2 + g)
        att_copy(seg, 0, g, None, 0, 6)

    @scoped
    def heads1(seg, g):
        att_wait(seg, att.at[seg, head_at(-1, c), g], g)
        att_copy(seg, -1, g, 0, 1, 4 + g)
        att_copy(seg, -1, g, None, 0, 7)
        att_wait(seg, att.at[seg, head_at(1, c), g], 2 + g)
        att_copy(seg, 1, g, 1, -1, 4 + g)
        att_copy(seg, 1, g, None, 0, 8)

    @scoped
    def heads2(seg, g):
        att_wait(seg, att.at[seg, head_at(2, c), g], 4 + g)
        att_copy(seg, 2, g, None, 0, 9)

    @scoped
    def heads3(seg, dz):
        att_wait(seg, att.at[seg, head_at(dz, other)], 6 + (0, -1, 1, 2).index(dz))

    def to_owners(seg):
        @pl.loop(1, 16)
        def _(p):
            who = (s + p) % 16
            remote(ps.at[seg, who], po.at[seg, s], ps_send.at[seg], po_recv.at[seg], (who, h)).start()

    @scoped
    def from_owners(seg):
        ref = po.at[seg, pl.ds(0, 15)]
        remote(ref, ref, ps_send.at[seg], po_recv.at[seg], ((s + 1) % 16, h)).wait_recv()

    def to_heads(ref, ssem, rsem, seg):
        @pl.loop(1, 8)
        def _(p):
            remote(ref.at[seg, h], ref.at[seg, h], ssem.at[seg], rsem.at[seg], (s, (h + p) % 8)).start()

    @scoped
    def from_heads(ref, ssem, rsem, seg):
        some = ref.at[seg, pl.ds(0, 7)]
        remote(some, some, ssem.at[seg], rsem.at[seg], (s, (h + 1) % 8)).wait_recv()

    def to_seq(seg):
        @pl.loop(1, 16)
        def _(p):
            remote(mb.at[seg, s], mb.at[seg, s], mb_send.at[seg], mb_recv.at[seg], ((s + p) % 16, h)).start()

    @scoped
    def from_seq(seg):
        ref = mb.at[seg, pl.ds(0, 15)]
        remote(ref, ref, mb_send.at[seg], mb_recv.at[seg], ((s + 1) % 16, h)).wait_recv()

    @scoped
    def all_sent():
        near = ((s + 1) % 16, h)
        for seg in range(2):
            groups = [
                (att.at[seg, pl.ds(0, 7)], att_send.at[seg]),
                (po.at[seg, pl.ds(0, 15)], ps_send.at[seg]),
                (mg.at[seg, pl.ds(0, 7)], mg_send.at[seg]),
                (pr.at[seg, pl.ds(0, 7)], pr_send.at[seg]),
            ]
            groups.append((mb.at[seg, pl.ds(0, 15)], mb_send.at[seg]))
            for ref, sem in groups:
                remote(ref, ref, sem, load_sem.at[0], near).wait_send()
        for (kind, seg), group in sent.items():
            for cond, rows in group.values():
                whole, rest = rows // 256, rows % 256
                refs = [kv.at[kind, seg, pl.ds(0, whole)]] if whole else []
                if rest:
                    refs.append(kv.at[kind, seg, 0, pl.ds(0, rest)])

                def wait(refs=refs, sem=kv_send.at[kind, seg]):
                    for ref in refs:
                        remote(ref, ref, sem, load_sem.at[0], near).wait_send()

                on(cond, wait)


    @scoped
    def norm_tokens(seg):
        gain = gain_ref[...].astype(F32).reshape(1, width)

        @pl.loop(0, tok // 16, unroll=2)
        def _(i):
            rows = pl.ds(pl.multiple_of(i * 16, 16), 16)
            v = xb[seg, rows, :].astype(F32)
            mean = jnp.sum(v * v, axis=-1, keepdims=True) * (1.0 / width)
            xn[seg, rows, :] = (v * lax.rsqrt(mean + 1e-06) * gain).astype(BF16)

    @scoped
    def keys_values(seg):
        kv[0, seg, s] = dot(xn[seg], wk[...]).astype(BF16)
        kv[1, seg, s] = dot(xn[seg], wv[...]).astype(BF16)

    @scoped
    def gather_memory(seg):
        m = lax.broadcasted_iota(jnp.int32, (32, 128), 0)
        j = lax.broadcasted_iota(jnp.int32, (32, 128), 1)
        blocks = mb[seg].reshape(128, 896)
        for yy in range(4):
            pick = (m == (j // 8) * 2 + j % 2) & ((j % 8) // 2 == yy)
            memb[:, 896 * yy:896 * yy + 896] = dot(jnp.where(pick, 1.0, 0.0).astype(BF16), blocks).astype(BF16)

    @scoped
    def project_memory(seg):
        gain = gain_ref[...].astype(F32).reshape(1, width)
        for pair in range(2):
            v = memb[pair * 16:pair * 16 + 16, :].astype(F32)
            mean = jnp.sum(v * v, axis=-1, keepdims=True) * (1.0 / width)
            nm[pair * 16:pair * 16 + 16, :] = (v * lax.rsqrt(mean + 1e-06) * gain).astype(BF16)
        qm[...] = dot(nm[...], wq[...]).astype(BF16)
        km[seg, 0:32, :] = dot(nm[...], wk[...]).astype(BF16)
        vm[seg, 0:32, :] = dot(nm[...], wv[...]).astype(BF16)

    def weights_of(scores, peak):
        return jnp.exp2((scores - peak) * EXP_FACTOR)

    def memory_scores(q, seg):
        lane = lax.broadcasted_iota(jnp.int32, (q.shape[0], 128), 1)
        return jnp.where(lane < 32, dot_t(q, km[seg]), NEG)

    @scoped
    def attend_memory(seg):
        q = jnp.concatenate([qm[:, 0:256], qm[:, 256:512]], axis=0)
        lane = lax.broadcasted_iota(jnp.int32, (64, 128), 1)
        first = jnp.where((lane < 32) & (s == 0), dot_t(q, km[seg]), NEG)
        scores = dot_t(q, kv[0, seg, s])
        peak = jnp.maximum(jnp.max(first, axis=1, keepdims=True), jnp.max(scores, axis=1, keepdims=True))
        w_first = weights_of(first, peak)
        w = weights_of(scores, peak)
        total = jnp.sum(w_first, axis=1, keepdims=True) + jnp.sum(w, axis=1, keepdims=True)
        mixed = dot(w_first.astype(BF16), vm[seg]) + dot(w.astype(BF16), kv[1, seg, s])
        stats = jnp.where(lane < 64, peak, total)
        for t in range(16):
            for g in range(2):
                row = 32 * g + 2 * t
                ps[seg, t, 2 * g:2 * g + 2, 0:256] = mixed[row:row + 2]
                ps[seg, t, 2 * g:2 * g + 2, 256:384] = stats[row:row + 2]
        po[seg, s] = ps[seg, s]

    @scoped
    def combine_memory(seg):
        peaks = [po[seg, t, :, 256:257] for t in range(16)]
        peak = peaks[0]
        for one in peaks[1:]:
            peak = jnp.maximum(peak, one)
        total = jnp.zeros((4, 1), F32)
        mixed = jnp.zeros((4, 256), F32)
        for t in range(16):
            f = weights_of(peaks[t], peak)
            total = total + f * po[seg, t, :, 320:321]
            mixed = mixed + f * po[seg, t, :, 0:256]
        result = mixed / total
        for g in range(2):
            mg[seg, h, :, 256 * g:256 * g + 256] = jnp.concatenate([result[2 * g:2 * g + 2]] * 4, axis=0).astype(BF16)

    @scoped
    def write_memory(seg):
        out = dot_t(mg[seg, 0], wo[:, 0:512])
        for head in range(1, 8):
            out = out + dot_t(mg[seg, head], wo[:, head * 512:head * 512 + 512])
        k = lax.broadcasted_iota(jnp.int32, (8, 32), 0)
        m = lax.broadcasted_iota(jnp.int32, (8, 32), 1)
        own = jnp.where(m == 2 * s + k % 2, 1.0, 0.0).astype(BF16)
        old = dot(own, memb[:, pl.ds(pl.multiple_of(z * 896, 128), 896)])
        old = jnp.where(c == 0, old[:, 0:cols], old[:, cols:2 * cols])
        part = dot((old + out).astype(BF16), mp[...])
        k = lax.broadcasted_iota(jnp.int32, (8, 896), 0)
        block = part[:, 0:896]
        for yy in range(1, 4):
            block = jnp.where(k // 2 == yy, part[:, 896 * yy:896 * yy + 896], block)
        pr[seg, h] = block.astype(BF16)

    @scoped
    def sum_memory(seg):
        total = pr[seg, 0].astype(F32)
        for head in range(1, 8):
            total = total + pr[seg, head].astype(F32)
        mb[seg, s] = total.astype(BF16)

    def first_keys(seg):
        docs = docs_ref[seg:seg + 1, :]
        pos = s * tok + lax.broadcasted_iota(jnp.int32, (tok, 1), 0)
        start = jnp.zeros((tok, 1), jnp.int32)
        for doc in (1, 2, 3):
            begin = jnp.sum(jnp.where(docs < doc, 1, 0), axis=1, keepdims=True)
            start = jnp.maximum(start, jnp.where(begin <= pos, begin, 0))
        return start, pos

    def score_blocks(seg, low, high):
        start, pos = first_keys(seg)

        @pl.loop(low, high)
        def _(d):
            t = s - d
            key_pos = t * tok + lax.broadcasted_iota(jnp.int32, (tok, tok), 1)
            ok = (key_pos >= start) & (key_pos <= pos)
            for g in range(2):
                scores = jnp.where(ok, dot_t(qb[seg, :, g * HD:g * HD + HD], kv[0, seg, t]), NEG)
                sc[g, d] = scores
                mxs[g] = jnp.maximum(mxs[g], jnp.maximum(scores[:, 0:128], scores[:, 128:256]))

    near = jnp.minimum(s, x + 4) + 1
    reach = jnp.minimum(s, 8) + 1

    @scoped
    def scores_near(seg):
        mxs[...] = jnp.full_like(mxs, NEG)
        score_blocks(seg, 0, near)

    @scoped
    def scores_far(seg):
        score_blocks(seg, near, reach)

    @scoped
    def attend(seg, g):
        first = memory_scores(qb[seg, :, g * HD:g * HD + HD], seg)
        peak = jnp.max(jnp.maximum(mxs[g], first), axis=1, keepdims=True)
        w_first = weights_of(first, peak)
        total = w_first
        mixed = dot(w_first.astype(BF16), vm[seg])
        for d in range(9):
            w = weights_of(sc[g, d], peak)
            if d > 0:
                w = jnp.where(d <= s, w, 0.0)
            total = total + (w[:, 0:128] + w[:, 128:256])
            mixed = mixed + dot(w.astype(BF16), kv[1, seg, jnp.maximum(s - d, 0)])
        total = jnp.sum(total, axis=1, keepdims=True)
        att[seg, h, g] = (mixed / total).astype(BF16)

    def head_term(seg, head, out):
        for g in range(2):
            lanes = pl.ds(pl.multiple_of(head * 512 + g * 256, 256), 256)
            out = out + dot_t(wo[:, lanes], att[seg, head, g])
        return out

    @scoped
    def add_heads(seg, *where):
        out = ha[seg]
        for dz, core in where:
            out = head_term(seg, head_at(dz, core), out)
        ha[seg] = out

    @scoped
    def last_heads(seg, *where):
        out = ha[seg]
        for dz, core in where:
            out = head_term(seg, head_at(dz, core), out)
        hid_ref[seg] = out.astype(BF16)

    @scoped
    def residual(seg):
        old = xr[seg].astype(F32).T
        ha[seg] = jnp.where(c == 0, old[0:cols], old[cols:2 * cols])

    km[...] = jnp.zeros_like(km)
    vm[...] = jnp.zeros_like(vm)
    with jax.named_scope("load0"):
        loads[8].wait()
        loads[0].wait()
    for k in (4, 3):
        loads[k].start()
    norm_tokens(0)
    with jax.named_scope("load1"):
        loads[1].wait()
        loads[2].wait()
    for k in (6, 5, 7, 10):
        loads[k].start()
    keys_values(0)
    with jax.named_scope("barrier"):
        pl.semaphore_wait(barrier, 22)
    round0(0, 0)
    with jax.named_scope("load4"):
        loads[4].wait()
        loads[9].wait()
    project_memory(0)
    attend_memory(0)
    to_owners(0)
    round0(0, 1)
    with jax.named_scope("load3"):
        loads[3].wait()
    norm_tokens(1)
    keys_values(1)
    from_owners(0)
    combine_memory(0)
    to_heads(mg, mg_send, mg_recv, 0)
    round1_keys(0)
    round1_values(0)
    with jax.named_scope("query"):
        qb[0] = dot(xn[0], wq[...]).astype(BF16)
    for k in (5, 6, 7, 10):
        loads[k].wait()
    from_heads(mg, mg_send, mg_recv, 0)
    write_memory(0)
    to_heads(pr, pr_send, pr_recv, 0)
    round2(0)
    from_heads(pr, pr_send, pr_recv, 0)
    sum_memory(0)
    to_seq(0)
    round0(1, 0, 1)
    with jax.named_scope("query"):
        qb[1] = dot(xn[1], wq[...]).astype(BF16)
    residual(0)
    residual(1)
    round3(0)
    scores_near(0)
    from_seq(0)
    gather_memory(0)
    project_memory(1)
    attend_memory(1)
    to_owners(1)
    round1_keys(1)
    round1_values(1)
    from_owners(1)
    combine_memory(1)
    to_heads(mg, mg_send, mg_recv, 1)
    round4(0)
    scores_far(0)
    attend(0, 0)
    heads0(0, 0)
    attend(0, 1)
    heads0(0, 1)
    round2(1)
    from_heads(mg, mg_send, mg_recv, 1)
    write_memory(1)
    to_heads(pr, pr_send, pr_recv, 1)
    heads1(0, 0)
    round3(1)
    heads1(0, 1)
    scores_near(1)
    round4(1)
    scores_far(1)
    attend(1, 0)
    heads0(1, 0)
    heads2(0, 0)
    attend(1, 1)
    heads0(1, 1)
    heads2(0, 1)
    from_heads(pr, pr_send, pr_recv, 1)
    sum_memory(1)
    to_seq(1)
    add_heads(0, (0, c), (-1, c), (1, c), (2, c))
    heads1(1, 0)
    for dz in (0, -1, 1, 2):
        heads3(0, dz)
    last_heads(0, (0, other), (-1, other), (1, other), (2, other))
    heads1(1, 1)
    add_heads(1, (0, c), (-1, c), (1, c))
    heads2(1, 0)
    from_seq(1)
    for dz in (0, -1, 1):
        heads3(1, dz)
    add_heads(1, (0, other), (-1, other), (1, other))
    heads2(1, 1)
    gather_memory(1)
    newmem_ref[...] = memb[...]
    add_heads(1, (2, c))
    heads3(1, 2)
    last_heads(1, (2, other))
    all_sent()


def per_device(segment_input, doc_ids, memory, gain, w_query, w_key, w_value, w_out, mem_proj):
    segs, tok, width = segment_input.shape
    cols = w_out.shape[1]
    anywhere = pl.BlockSpec(memory_space=pl.ANY)
    vmem = pl.BlockSpec(memory_space=pltpu.VMEM)
    dma = pltpu.SemaphoreType.DMA
    hidden_t, new_memory = pl.pallas_call(
        body,
        out_shape=(
            pltpu.VMEM((segs, cols, tok), BF16),
            pltpu.VMEM(memory.shape, BF16),
        ),
        in_specs=[anywhere] * 9,
        out_specs=(vmem, vmem),
        scratch_shapes=[
            pltpu.VMEM(doc_ids.shape, jnp.int32),
            pltpu.VMEM(gain.shape, BF16),
            pltpu.VMEM((segs, tok, width), BF16),
            pltpu.VMEM((segs, tok, width), BF16),
            pltpu.VMEM((segs, tok, 896), BF16),
            pltpu.VMEM(w_query.shape, BF16),
            pltpu.VMEM(w_key.shape, BF16),
            pltpu.VMEM(w_value.shape, BF16),
            pltpu.VMEM((cols, w_out.shape[0]), BF16),
            pltpu.VMEM(mem_proj.shape, BF16),
            pltpu.VMEM((segs, tok, 2 * HD), BF16),
            pltpu.VMEM((2, segs, 16, tok, HD), BF16),
            pltpu.VMEM((segs, 128, HD), BF16),
            pltpu.VMEM((segs, 128, HD), BF16),
            pltpu.VMEM((32, width), BF16),
            pltpu.VMEM((32, width), BF16),
            pltpu.VMEM((32, 2 * HD), BF16),
            pltpu.VMEM((2, 9, tok, tok), F32),
            pltpu.VMEM((2, tok, 128), F32),
            pltpu.VMEM((segs, 8, 2, tok, HD), BF16),
            pltpu.VMEM((segs, cols, tok), F32),
            pltpu.VMEM((segs, 16, 4, 384), F32),
            pltpu.VMEM((segs, 16, 4, 384), F32),
            pltpu.VMEM((segs, 8, 8, 2 * HD), BF16),
            pltpu.VMEM((segs, 8, 8, 896), BF16),
            pltpu.VMEM((segs, 16, 8, 896), BF16),
            dma((11,)),
            dma((2, segs)),
            dma((2, segs, 12)),
            dma((segs,)),
            dma((segs, 10)),
            dma((segs,)),
            dma((segs,)),
            dma((segs,)),
            dma((segs,)),
            dma((segs,)),
            dma((segs,)),
            dma((segs,)),
            dma((segs,)),
        ],
        compiler_params=pltpu.CompilerParams(
            collective_id=0, has_side_effects=True, vmem_limit_bytes=60000 * 1024),
    )(segment_input, doc_ids, memory, gain, w_query, w_key, w_value, w_out.T, mem_proj)
    return hidden_t.transpose(0, 2, 1), new_memory


def solution(mesh):
    return jax.shard_map(
        per_device,
        mesh=mesh,
        in_specs=(
            P(None, "seq", None),
            P(),
            P(),
            P(),
            P(None, "head"),
            P(None, "head"),
            P(None, "head"),
            P(None, "head"),
            P("head", None),
        ),
        out_specs=(P(None, "seq", "head"), P()),
        check_vma=False,
    )
```

```python
import math

import jax
import jax.numpy as jnp
from jax import lax
from jax.experimental import pallas as pl
from jax.experimental.pallas import tpu as pltpu
from jax.sharding import PartitionSpec as P

HD = 256
MESH = pl.DeviceIdType.MESH
F32 = jnp.float32
BF16 = jnp.bfloat16
NEG = -1e30
EXP_FACTOR = HD ** (-0.5) * math.log2(math.e)


def scoped(f):
    def g(*args):
        with jax.named_scope(f.__name__ + "".join(f"_{a}" for a in args if isinstance(a, int))):
            return f(*args)
    return g


def dot(a, b):
    return jnp.dot(a, b, preferred_element_type=F32)


def dot_t(a, b):
    return lax.dot_general(a, b, (((1,), (1,)), ((), ())), preferred_element_type=F32)


def body(
    x_hbm, docs_hbm, mem_hbm, gain_hbm, wq_hbm, wk_hbm, wv_hbm, wo_hbm, mp_hbm,
    hid_ref, newmem_ref,
    docs_ref, gain_ref, xb, xn, xr, wq, wk, wv, wo, mp, qb, kv, km, vm, nm, memb, qm, sc, mxs, att, ha, ps, po, mg, pr, mb,
    load_sem, kv_send, kv_recv, att_send, att_recv, ps_send, po_recv, mg_send, mg_recv, pr_send, pr_recv, mb_send, mb_recv,
):
    segs, tok, width = x_hbm.shape
    s = lax.axis_index("seq")
    h = lax.axis_index("head")
    y, x = s // 4, s % 4
    z, c = h // 2, h % 2
    cols = wo_hbm.shape[0]

    loads = [
        pltpu.make_async_copy(x_hbm.at[0, pl.ds(0, 128)], xb.at[0, pl.ds(0, 128)], load_sem.at[0]),
        pltpu.make_async_copy(wk_hbm, wk, load_sem.at[1]),
        pltpu.make_async_copy(wv_hbm, wv, load_sem.at[2]),
        pltpu.make_async_copy(x_hbm.at[1], xb.at[1], load_sem.at[3]),
        pltpu.make_async_copy(wq_hbm, wq, load_sem.at[4]),
        pltpu.make_async_copy(mp_hbm, mp, load_sem.at[5]),
        pltpu.make_async_copy(wo_hbm, wo, load_sem.at[6]),
        pltpu.make_async_copy(
            x_hbm.at[:, :, pl.ds(pl.multiple_of(z * 896, 128), 896)], xr, load_sem.at[7]),
    ]
    loads += [
        pltpu.make_async_copy(gain_hbm, gain_ref, load_sem.at[8]),
        pltpu.make_async_copy(mem_hbm, memb, load_sem.at[9]),
        pltpu.make_async_copy(docs_hbm, docs_ref, load_sem.at[10]),
        pltpu.make_async_copy(x_hbm.at[0, pl.ds(128, 128)], xb.at[0, pl.ds(128, 128)], load_sem.at[11]),
    ]
    for k in (8, 0, 11, 1, 2, 9):
        loads[k].start()

    barrier = pltpu.get_barrier_semaphore()

    @pl.loop(1, 16)
    def _(p):
        pl.semaphore_signal(barrier, inc=1, device_id=((s + p) % 16, h), device_id_type=MESH)

    @pl.loop(1, 8)
    def _(p):
        pl.semaphore_signal(barrier, inc=1, device_id=(s, (h + p) % 8), device_id_type=MESH)

    def remote(src, dst, ssem, rsem, where):
        return pltpu.make_async_remote_copy(
            src_ref=src, dst_ref=dst, send_sem=ssem, recv_sem=rsem, device_id=where, device_id_type=MESH)

    def at(kind, i, j):
        dx, dy = (i, j) if kind == 0 else (j, i)
        return ((y + dy + 4) % 4) * 4 + (x + dx + 4) % 4

    not_last = y <= 2
    early = y <= 1
    middle = (y >= 1) & (y <= 2)
    relay = (y == 0) | (y == 3)
    has_one = y >= 1
    has_two = y >= 2
    sent = {}

    def on(cond, f):
        if cond is None:
            f()
        else:
            pl.when(cond)(f)

    def cut_rows(kind, along):
        return 96 if (kind == 0) == (along == 2) else 128

    def piece(kind, seg, i, j, half, along):
        ref = kv.at[kind, seg, at(kind, i, j)]
        at_row = cut_rows(kind, along)
        if half is None:
            return ref, 256
        if half == 0:
            return ref.at[pl.ds(0, at_row)], at_row
        return ref.at[pl.ds(at_row, 256 - at_row)], 256 - at_row

    slots = (
        {(-1, 0): 0, (1, 0): 1, (2, 0): 2, (0, -1): 3, (-1, -1): 4, (1, -1): 5, (2, -1): 6, (0, 1): 7,
         (-1, 1): 8, (1, 1): 9, (2, 1): 10, (0, 2): 11, (-1, 2): 11, (1, 2): 11, (2, 2): 11},
        {(-1, 0): 0, (1, 0): 1, (2, 0): 2, (0, -1): 3, (0, 1): 4, (-1, -1): 5, (-1, 1): 6, (2, -1): 7,
         (2, 1): 8, (0, 2): 9, (-1, 2): 10, (2, 2): 11},
    )

    def seen(kind, i, j):
        return slots[kind][((i + 5) % 4 - 1, (j + 5) % 4 - 1)]

    def kv_copy(kind, seg, i, j, half, di, dj, name=None, cond=None):
        ref, rows = piece(kind, seg, i, j, half, 1 if di else 2)
        group = sent.setdefault((kind, seg), {})
        group[name] = (cond, group.get(name, (cond, 0))[1] + rows)
        on(cond, lambda: remote(
            ref, ref, kv_send.at[kind, seg], kv_recv.at[kind, seg, seen(kind, i - di, j - dj)],
            (at(kind, di, dj), h)).start())

    def kv_wait(kind, seg, i, j, cond=None, half=None):
        ref, _ = piece(kind, seg, i, j, half, 1 if j == 0 else 2)

        def wait(ref=ref):
            remote(ref, ref, kv_send.at[kind, seg], kv_recv.at[kind, seg, seen(kind, i, j)],
                   (at(kind, 1, 0), h)).wait_recv()

        on(cond, wait)

    def up_down(seg, i):
        kv_copy(0, seg, i, 0, None, 0, 1, "not_last", not_last)
        kv_copy(0, seg, i, 0, 1, 0, -1, "early", early)

    def relay_keys(seg, i):
        kv_wait(0, seg, i, -1, has_one)
        kv_copy(0, seg, i, -1, 0, 0, 1, "middle", middle)
        kv_wait(0, seg, i, 1, relay, 1)
        kv_copy(0, seg, i, 1, 1, 0, -1, "relay", relay)

    def relay_values(seg, i, name, cond):
        kv_wait(1, seg, i, -1, cond)
        kv_copy(1, seg, i, -1, 0, 0, 1, name, cond)
        kv_wait(1, seg, i, 1, cond)
        kv_copy(1, seg, i, 1, 1, 0, -1, name, cond)

    def both_sides(kind, seg, i, name, cond):
        di, dj = (1, 0) if kind == 0 else (0, 1)
        kv_copy(kind, seg, i, 0, None, di, dj, name, cond)
        kv_copy(kind, seg, i, 0, None, -di, -dj, name, cond)

    @scoped
    def round0(seg, *kinds):
        if 0 in kinds:
            both_sides(0, seg, 0, None, None)
            up_down(seg, 0)
        if 1 in kinds:
            kv_copy(1, seg, 0, 0, None, 1, 0, "not_last", not_last)
            kv_copy(1, seg, 0, 0, 1, -1, 0, "early", early)
            both_sides(1, seg, 0, None, None)

    @scoped
    def round1_keys(seg):
        kv_wait(0, seg, -1, 0)
        kv_copy(0, seg, -1, 0, 0, 1, 0)
        up_down(seg, -1)
        kv_wait(0, seg, 1, 0)
        kv_copy(0, seg, 1, 0, 1, -1, 0)
        up_down(seg, 1)
        relay_keys(seg, 0)

    @scoped
    def round1_values(seg):
        kv_wait(1, seg, -1, 0, has_one)
        kv_copy(1, seg, -1, 0, 0, 1, 0, "middle", middle)
        both_sides(1, seg, -1, "has_one", has_one)
        kv_wait(1, seg, 1, 0, relay, 1)
        kv_copy(1, seg, 1, 0, 1, -1, 0, "relay", relay)
        relay_values(seg, 0, None, None)

    @scoped
    def round2(seg):
        kv_wait(0, seg, 2, 0)
        up_down(seg, 2)
        kv_wait(1, seg, 2, 0, has_two)
        both_sides(1, seg, 2, "has_two", has_two)
        relay_keys(seg, -1)
        relay_keys(seg, 1)
        relay_values(seg, -1, "has_one", has_one)

    @scoped
    def round3(seg):
        relay_keys(seg, 2)
        relay_values(seg, 2, "has_two", has_two)

    @scoped
    def round4(seg):
        @pl.when(has_two)
        def _():
            ref = kv.at[0, seg, pl.ds(0, 4)]
            remote(ref, ref, kv_send.at[0, seg], kv_recv.at[0, seg, 11], (at(0, 1, 0), h)).wait_recv()

        kv_wait(1, seg, 0, 2)
        kv_wait(1, seg, -1, 2, has_one)
        kv_wait(1, seg, 2, 2, has_two)

    def head_at(dz, core):
        return ((z + dz + 4) % 4) * 2 + core

    other = 1 - c

    def att_piece(seg, head, g, half):
        ref = att.at[seg, head, g]
        return ref if half is None else ref.at[pl.ds(half * 128, 128)]

    def att_copy(seg, dz, g, half, to, slot):
        head, where = head_at(dz, c), head_at(to, c if slot < 6 else other)
        ref = att_piece(seg, head, g, half)
        remote(ref, ref, att_send.at[seg], att_recv.at[seg, slot], (s, where)).start()

    def att_wait(seg, ref, slot):
        remote(ref, ref, att_send.at[seg], att_recv.at[seg, slot], (s, head_at(1, c))).wait_recv()

    @scoped
    def heads0(seg, g):
        att_copy(seg, 0, g, None, 1, g)
        att_copy(seg, 0, g, None, -1, 2 + g)
        att_copy(seg, 0, g, None, 0, 6)

    @scoped
    def heads1(seg, g):
        att_wait(seg, att.at[seg, head_at(-1, c), g], g)
        att_copy(seg, -1, g, 0, 1, 4 + g)
        att_copy(seg, -1, g, None, 0, 7)
        att_wait(seg, att.at[seg, head_at(1, c), g], 2 + g)
        att_copy(seg, 1, g, 1, -1, 4 + g)
        att_copy(seg, 1, g, None, 0, 8)

    @scoped
    def heads2(seg, g):
        att_wait(seg, att.at[seg, head_at(2, c), g], 4 + g)
        att_copy(seg, 2, g, None, 0, 9)

    @scoped
    def heads3(seg, dz):
        att_wait(seg, att.at[seg, head_at(dz, other)], 6 + (0, -1, 1, 2).index(dz))

    def to_owners(seg):
        @pl.loop(1, 16)
        def _(p):
            who = (s + p) % 16
            remote(ps.at[seg, who], po.at[seg, s], ps_send.at[seg], po_recv.at[seg], (who, h)).start()

    @scoped
    def from_owners(seg):
        ref = po.at[seg, pl.ds(0, 15)]
        remote(ref, ref, ps_send.at[seg], po_recv.at[seg], ((s + 1) % 16, h)).wait_recv()

    def to_heads(ref, ssem, rsem, seg):
        @pl.loop(1, 8)
        def _(p):
            remote(ref.at[seg, h], ref.at[seg, h], ssem.at[seg], rsem.at[seg], (s, (h + p) % 8)).start()

    @scoped
    def from_heads(ref, ssem, rsem, seg):
        some = ref.at[seg, pl.ds(0, 7)]
        remote(some, some, ssem.at[seg], rsem.at[seg], (s, (h + 1) % 8)).wait_recv()

    def to_seq(seg):
        @pl.loop(1, 16)
        def _(p):
            remote(mb.at[seg, s], mb.at[seg, s], mb_send.at[seg], mb_recv.at[seg], ((s + p) % 16, h)).start()

    @scoped
    def from_seq(seg):
        ref = mb.at[seg, pl.ds(0, 15)]
        remote(ref, ref, mb_send.at[seg], mb_recv.at[seg], ((s + 1) % 16, h)).wait_recv()

    @scoped
    def all_sent():
        near = ((s + 1) % 16, h)
        for seg in range(2):
            groups = [
                (att.at[seg, pl.ds(0, 7)], att_send.at[seg]),
                (po.at[seg, pl.ds(0, 15)], ps_send.at[seg]),
                (mg.at[seg, pl.ds(0, 7)], mg_send.at[seg]),
                (pr.at[seg, pl.ds(0, 7)], pr_send.at[seg]),
            ]
            groups.append((mb.at[seg, pl.ds(0, 15)], mb_send.at[seg]))
            for ref, sem in groups:
                remote(ref, ref, sem, load_sem.at[0], near).wait_send()
        for (kind, seg), group in sent.items():
            for cond, rows in group.values():
                whole, rest = rows // 256, rows % 256
                refs = [kv.at[kind, seg, pl.ds(0, whole)]] if whole else []
                if rest:
                    refs.append(kv.at[kind, seg, 0, pl.ds(0, rest)])

                def wait(refs=refs, sem=kv_send.at[kind, seg]):
                    for ref in refs:
                        remote(ref, ref, sem, load_sem.at[0], near).wait_send()

                on(cond, wait)


    @scoped
    def norm_tokens(seg, low, high):
        gain = gain_ref[...].astype(F32).reshape(1, width)

        @pl.loop(low // 16, high // 16, unroll=4)
        def _(i):
            rows = pl.ds(pl.multiple_of(i * 16, 16), 16)
            v = xb[seg, rows, :].astype(F32)
            mean = jnp.sum(v * v, axis=-1, keepdims=True) * (1.0 / width)
            xn[seg, rows, :] = (v * lax.rsqrt(mean + 1e-06) * gain).astype(BF16)

    @scoped
    def keys_values(seg):
        kv[0, seg, s] = dot(xn[seg], wk[...]).astype(BF16)
        kv[1, seg, s] = dot(xn[seg], wv[...]).astype(BF16)

    @scoped
    def gather_memory(seg):
        m = lax.broadcasted_iota(jnp.int32, (32, 128), 0)
        j = lax.broadcasted_iota(jnp.int32, (32, 128), 1)
        blocks = mb[seg].reshape(128, 896)
        for yy in range(4):
            pick = (m == (j // 8) * 2 + j % 2) & ((j % 8) // 2 == yy)
            memb[:, 896 * yy:896 * yy + 896] = dot(jnp.where(pick, 1.0, 0.0).astype(BF16), blocks).astype(BF16)

    @scoped
    def project_memory(seg):
        gain = gain_ref[...].astype(F32).reshape(1, width)
        for pair in range(2):
            v = memb[pair * 16:pair * 16 + 16, :].astype(F32)
            mean = jnp.sum(v * v, axis=-1, keepdims=True) * (1.0 / width)
            nm[pair * 16:pair * 16 + 16, :] = (v * lax.rsqrt(mean + 1e-06) * gain).astype(BF16)
        qm[...] = dot(nm[...], wq[...]).astype(BF16)
        km[seg, 0:32, :] = dot(nm[...], wk[...]).astype(BF16)
        vm[seg, 0:32, :] = dot(nm[...], wv[...]).astype(BF16)

    def weights_of(scores, peak):
        return jnp.exp2((scores - peak) * EXP_FACTOR)

    def memory_scores(q, seg):
        lane = lax.broadcasted_iota(jnp.int32, (q.shape[0], 128), 1)
        return jnp.where(lane < 32, dot_t(q, km[seg]), NEG)

    @scoped
    def attend_memory(seg):
        q = jnp.concatenate([qm[:, 0:256], qm[:, 256:512]], axis=0)
        lane = lax.broadcasted_iota(jnp.int32, (64, 128), 1)
        first = jnp.where((lane < 32) & (s == 0), dot_t(q, km[seg]), NEG)
        scores = dot_t(q, kv[0, seg, s])
        peak = jnp.maximum(jnp.max(first, axis=1, keepdims=True), jnp.max(scores, axis=1, keepdims=True))
        w_first = weights_of(first, peak)
        w = weights_of(scores, peak)
        total = jnp.sum(w_first, axis=1, keepdims=True) + jnp.sum(w, axis=1, keepdims=True)
        mixed = dot(w_first.astype(BF16), vm[seg]) + dot(w.astype(BF16), kv[1, seg, s])
        stats = jnp.where(lane < 64, peak, total)
        for t in range(16):
            for g in range(2):
                row = 32 * g + 2 * t
                ps[seg, t, 2 * g:2 * g + 2, 0:256] = mixed[row:row + 2]
                ps[seg, t, 2 * g:2 * g + 2, 256:384] = stats[row:row + 2]
        po[seg, s] = ps[seg, s]

    @scoped
    def combine_memory(seg):
        peaks = [po[seg, t, :, 256:257] for t in range(16)]
        peak = peaks[0]
        for one in peaks[1:]:
            peak = jnp.maximum(peak, one)
        total = jnp.zeros((4, 1), F32)
        mixed = jnp.zeros((4, 256), F32)
        for t in range(16):
            f = weights_of(peaks[t], peak)
            total = total + f * po[seg, t, :, 320:321]
            mixed = mixed + f * po[seg, t, :, 0:256]
        result = mixed / total
        for g in range(2):
            mg[seg, h, :, 256 * g:256 * g + 256] = jnp.concatenate([result[2 * g:2 * g + 2]] * 4, axis=0).astype(BF16)

    @scoped
    def write_memory(seg):
        out = dot_t(mg[seg, 0], wo[:, 0:512])
        for head in range(1, 8):
            out = out + dot_t(mg[seg, head], wo[:, head * 512:head * 512 + 512])
        k = lax.broadcasted_iota(jnp.int32, (8, 32), 0)
        m = lax.broadcasted_iota(jnp.int32, (8, 32), 1)
        own = jnp.where(m == 2 * s + k % 2, 1.0, 0.0).astype(BF16)
        old = dot(own, memb[:, pl.ds(pl.multiple_of(z * 896, 128), 896)])
        old = jnp.where(c == 0, old[:, 0:cols], old[:, cols:2 * cols])
        part = dot((old + out).astype(BF16), mp[...])
        k = lax.broadcasted_iota(jnp.int32, (8, 896), 0)
        block = part[:, 0:896]
        for yy in range(1, 4):
            block = jnp.where(k // 2 == yy, part[:, 896 * yy:896 * yy + 896], block)
        pr[seg, h] = block.astype(BF16)

    @scoped
    def sum_memory(seg):
        total = pr[seg, 0].astype(F32)
        for head in range(1, 8):
            total = total + pr[seg, head].astype(F32)
        mb[seg, s] = total.astype(BF16)

    def first_keys(seg):
        docs = docs_ref[seg:seg + 1, :]
        pos = s * tok + lax.broadcasted_iota(jnp.int32, (tok, 1), 0)
        start = jnp.zeros((tok, 1), jnp.int32)
        for doc in (1, 2, 3):
            begin = jnp.sum(jnp.where(docs < doc, 1, 0), axis=1, keepdims=True)
            start = jnp.maximum(start, jnp.where(begin <= pos, begin, 0))
        return start, pos

    def score_blocks(seg, low, high):
        start, pos = first_keys(seg)

        @pl.loop(low, high)
        def _(d):
            t = s - d
            key_pos = t * tok + lax.broadcasted_iota(jnp.int32, (tok, tok), 1)
            ok = (key_pos >= start) & (key_pos <= pos)
            for g in range(2):
                scores = jnp.where(ok, dot_t(qb[seg, :, g * HD:g * HD + HD], kv[0, seg, t]), NEG)
                sc[g, d] = scores
                mxs[g] = jnp.maximum(mxs[g], jnp.maximum(scores[:, 0:128], scores[:, 128:256]))

    near = jnp.minimum(s, x + 4) + 1
    reach = jnp.minimum(s, 8) + 1

    @scoped
    def scores_near(seg):
        mxs[...] = jnp.full_like(mxs, NEG)
        score_blocks(seg, 0, near)

    @scoped
    def scores_far(seg):
        score_blocks(seg, near, reach)

    @scoped
    def attend(seg, g):
        first = memory_scores(qb[seg, :, g * HD:g * HD + HD], seg)
        peak = jnp.max(jnp.maximum(mxs[g], first), axis=1, keepdims=True)
        w_first = weights_of(first, peak)
        total = w_first
        mixed = dot(w_first.astype(BF16), vm[seg])
        for d in range(9):
            w = weights_of(sc[g, d], peak)
            if d > 0:
                w = jnp.where(d <= s, w, 0.0)
            total = total + (w[:, 0:128] + w[:, 128:256])
            mixed = mixed + dot(w.astype(BF16), kv[1, seg, jnp.maximum(s - d, 0)])
        total = jnp.sum(total, axis=1, keepdims=True)
        att[seg, h, g] = (mixed / total).astype(BF16)

    def head_term(seg, head, out):
        for g in range(2):
            lanes = pl.ds(pl.multiple_of(head * 512 + g * 256, 256), 256)
            out = out + dot_t(wo[:, lanes], att[seg, head, g])
        return out

    @scoped
    def add_heads(seg, *where):
        out = ha[seg]
        for dz, core in where:
            out = head_term(seg, head_at(dz, core), out)
        ha[seg] = out

    @scoped
    def last_heads(seg, *where):
        out = ha[seg]
        for dz, core in where:
            out = head_term(seg, head_at(dz, core), out)
        hid_ref[seg] = out.astype(BF16)

    @scoped
    def residual(seg):
        old = xr[seg].astype(F32).T
        ha[seg] = jnp.where(c == 0, old[0:cols], old[cols:2 * cols])

    km[...] = jnp.zeros_like(km)
    vm[...] = jnp.zeros_like(vm)
    with jax.named_scope("load0"):
        loads[8].wait()
        loads[0].wait()
    for k in (4, 3):
        loads[k].start()
    norm_tokens(0, 0, 128)
    loads[11].wait()
    norm_tokens(0, 128, 256)
    with jax.named_scope("load1"):
        loads[1].wait()
        loads[2].wait()
    for k in (6, 5, 7, 10):
        loads[k].start()
    keys_values(0)
    with jax.named_scope("barrier"):
        pl.semaphore_wait(barrier, 22)
    round0(0, 0)
    with jax.named_scope("load4"):
        loads[4].wait()
        loads[9].wait()
    project_memory(0)
    attend_memory(0)
    to_owners(0)
    round0(0, 1)
    with jax.named_scope("load3"):
        loads[3].wait()
    norm_tokens(1, 0, 256)
    keys_values(1)
    from_owners(0)
    combine_memory(0)
    to_heads(mg, mg_send, mg_recv, 0)
    round1_keys(0)
    round1_values(0)
    with jax.named_scope("query"):
        qb[0] = dot(xn[0], wq[...]).astype(BF16)
    for k in (5, 6, 7, 10):
        loads[k].wait()
    from_heads(mg, mg_send, mg_recv, 0)
    write_memory(0)
    to_heads(pr, pr_send, pr_recv, 0)
    round2(0)
    from_heads(pr, pr_send, pr_recv, 0)
    sum_memory(0)
    to_seq(0)
    round0(1, 0, 1)
    with jax.named_scope("query"):
        qb[1] = dot(xn[1], wq[...]).astype(BF16)
    residual(0)
    residual(1)
    round3(0)
    scores_near(0)
    from_seq(0)
    gather_memory(0)
    project_memory(1)
    attend_memory(1)
    to_owners(1)
    round1_keys(1)
    round1_values(1)
    from_owners(1)
    combine_memory(1)
    to_heads(mg, mg_send, mg_recv, 1)
    round4(0)
    scores_far(0)
    attend(0, 0)
    heads0(0, 0)
    attend(0, 1)
    heads0(0, 1)
    round2(1)
    from_heads(mg, mg_send, mg_recv, 1)
    write_memory(1)
    to_heads(pr, pr_send, pr_recv, 1)
    heads1(0, 0)
    round3(1)
    heads1(0, 1)
    scores_near(1)
    round4(1)
    scores_far(1)
    attend(1, 0)
    heads0(1, 0)
    heads2(0, 0)
    attend(1, 1)
    heads0(1, 1)
    heads2(0, 1)
    from_heads(pr, pr_send, pr_recv, 1)
    sum_memory(1)
    to_seq(1)
    add_heads(0, (0, c), (-1, c), (1, c), (2, c))
    heads1(1, 0)
    for dz in (0, -1, 1, 2):
        heads3(0, dz)
    last_heads(0, (0, other), (-1, other), (1, other), (2, other))
    heads1(1, 1)
    add_heads(1, (0, c), (-1, c), (1, c))
    heads2(1, 0)
    from_seq(1)
    for dz in (0, -1, 1):
        heads3(1, dz)
    add_heads(1, (0, other), (-1, other), (1, other))
    heads2(1, 1)
    gather_memory(1)
    newmem_ref[...] = memb[...]
    add_heads(1, (2, c))
    heads3(1, 2)
    last_heads(1, (2, other))
    all_sent()


def per_device(segment_input, doc_ids, memory, gain, w_query, w_key, w_value, w_out, mem_proj):
    segs, tok, width = segment_input.shape
    cols = w_out.shape[1]
    anywhere = pl.BlockSpec(memory_space=pl.ANY)
    vmem = pl.BlockSpec(memory_space=pltpu.VMEM)
    dma = pltpu.SemaphoreType.DMA
    hidden_t, new_memory = pl.pallas_call(
        body,
        out_shape=(
            pltpu.VMEM((segs, cols, tok), BF16),
            pltpu.VMEM(memory.shape, BF16),
        ),
        in_specs=[anywhere] * 9,
        out_specs=(vmem, vmem),
        scratch_shapes=[
            pltpu.VMEM(doc_ids.shape, jnp.int32),
            pltpu.VMEM(gain.shape, BF16),
            pltpu.VMEM((segs, tok, width), BF16),
            pltpu.VMEM((segs, tok, width), BF16),
            pltpu.VMEM((segs, tok, 896), BF16),
            pltpu.VMEM(w_query.shape, BF16),
            pltpu.VMEM(w_key.shape, BF16),
            pltpu.VMEM(w_value.shape, BF16),
            pltpu.VMEM((cols, w_out.shape[0]), BF16),
            pltpu.VMEM(mem_proj.shape, BF16),
            pltpu.VMEM((segs, tok, 2 * HD), BF16),
            pltpu.VMEM((2, segs, 16, tok, HD), BF16),
            pltpu.VMEM((segs, 128, HD), BF16),
            pltpu.VMEM((segs, 128, HD), BF16),
            pltpu.VMEM((32, width), BF16),
            pltpu.VMEM((32, width), BF16),
            pltpu.VMEM((32, 2 * HD), BF16),
            pltpu.VMEM((2, 9, tok, tok), F32),
            pltpu.VMEM((2, tok, 128), F32),
            pltpu.VMEM((segs, 8, 2, tok, HD), BF16),
            pltpu.VMEM((segs, cols, tok), F32),
            pltpu.VMEM((segs, 16, 4, 384), F32),
            pltpu.VMEM((segs, 16, 4, 384), F32),
            pltpu.VMEM((segs, 8, 8, 2 * HD), BF16),
            pltpu.VMEM((segs, 8, 8, 896), BF16),
            pltpu.VMEM((segs, 16, 8, 896), BF16),
            dma((12,)),
            dma((2, segs)),
            dma((2, segs, 12)),
            dma((segs,)),
            dma((segs, 10)),
            dma((segs,)),
            dma((segs,)),
            dma((segs,)),
            dma((segs,)),
            dma((segs,)),
            dma((segs,)),
            dma((segs,)),
            dma((segs,)),
        ],
        compiler_params=pltpu.CompilerParams(
            collective_id=0, has_side_effects=True, vmem_limit_bytes=60000 * 1024),
    )(segment_input, doc_ids, memory, gain, w_query, w_key, w_value, w_out.T, mem_proj)
    return hidden_t.transpose(0, 2, 1), new_memory


def solution(mesh):
    return jax.shard_map(
        per_device,
        mesh=mesh,
        in_specs=(
            P(None, "seq", None),
            P(),
            P(),
            P(),
            P(None, "head"),
            P(None, "head"),
            P(None, "head"),
            P(None, "head"),
            P("head", None),
        ),
        out_specs=(P(None, "seq", "head"), P()),
        check_vma=False,
    )
```
